32 devices in a mesh: seq: 4 (over z), tensor: 2 (over x), dp: 4 (over y, core).
Axes of the slice: x: 2, y: 2, z: 4, core: 2. Of those that a mesh axis runs over, the one named last changes fastest.
Arguments:
- tokens: bfloat16 [4, 1024, 3072], P('dp', 'seq'), may hold values from -6 to 6
- cotangent: bfloat16 [4, 1024, 3072], P('dp', 'seq'), may hold values from -6 to 6
- qkv_weight: bfloat16 [3072, 3, 768], P(('seq', 'dp'), None, 'tensor'), may hold values from -0.109375 to 0.109375
- out_weight: bfloat16 [3072, 768], P(('seq', 'dp'), 'tensor'), may hold values from -0.21875 to 0.21875
Outputs:
- qkv_grad: float32 [3072, 3, 768], P(('seq', 'dp'), None, 'tensor')
- out_grad: float32 [3072, 768], P(('seq', 'dp'), 'tensor')
- branch_grad: bfloat16 [4, 1024, 3072], P('dp', 'seq', 'tensor')
The draws below stay inside these ranges and needn't reach their ends.
All inputs are finite; a program needn't handle non-finite values.
Results may differ from the reference program's by a relative error of at most 0.025.
Values may be sent and summed in bfloat16 or wider, within the bound.
A program may use at most 128 MiB of HBM per device.

```python
import jax
import jax.numpy as jnp
from jax import lax

D = 3072
HD = 128
TOK_DEV = 256
HEADS = 6
SEQ_LEN = 1024
BATCH = 4
N_SEQ = 4


def strengthened(drawn, key, source, target, blocks, factor):
    def block_of(axis_at):
        return (jnp.arange(drawn.shape[axis_at]) // (drawn.shape[axis_at] // blocks)).reshape((-1,) + (1,) * (drawn.ndim - 1 - axis_at))

    near = jax.random.permutation(key, blocks)[block_of(target)]
    second = (block_of(target) + blocks // 2) % blocks
    return jnp.where((block_of(source) == near) | (block_of(source) == second), factor * drawn, drawn)


def block_scale(stream_key, dims, shards, low, largest):
    loudness = 1.0
    for axis_at, blocks in shards:
        draws = jax.random.uniform(jax.random.fold_in(jax.random.fold_in(stream_key, 6), axis_at), (blocks,), jnp.float32, low / len(shards), largest / len(shards))
        loudness = loudness * jnp.repeat(jnp.exp(draws), dims[axis_at] // blocks).reshape((-1,) + (1,) * (len(dims) - 1 - axis_at))
    return loudness


def bell_draw(stream_key, extent, scale, most, split=(), held_as=jnp.bfloat16):
    values = jax.random.normal(stream_key, extent, jnp.float32) * scale
    if len(split) > 0:
        values = block_scale(stream_key, extent, split, -0.22, 0.18) * values
    return jnp.clip(values, min=-most, max=most).astype(held_as)


def bell_draw_with(rng, extent, scale, reach, shards, heavy, kind=jnp.bfloat16):
    result = scale * jax.random.normal(rng, extent, jnp.float32)
    if shards:
        result = result * block_scale(rng, extent, shards, -0.22, 0.18)
    return jnp.clip(strengthened(result, jax.random.fold_in(rng, 3), *heavy), -reach, reach).astype(kind)


def setup_inputs(seed: int = 0) -> dict:
    seeds = jax.random.split(jax.random.key(seed), 5)
    return {
        "tokens": bell_draw_with(seeds[0], (BATCH, SEQ_LEN, D), 1.0, 6.0, ((0, 4), (1, 4)), (1, 2, 4, 2.0)),
        "cotangent": bell_draw_with(seeds[1], (BATCH, SEQ_LEN, D), 1.0, 6.0, ((0, 4), (1, 4)), (1, 2, 4, 2.0)),
        "qkv_weight": bell_draw(seeds[2], (D, 3, HEADS * HD), D ** -0.5, 0.109375, ((0, 16), (2, 2))),
        "out_weight": bell_draw(seeds[3], (D, HEADS * HD), (HEADS * HD) ** -0.5, 0.21875, ((0, 16), (1, 2))),
    }


epsilon = 1e-06

def normalize(values):
    average = lax.optimization_barrier(jnp.mean(values, axis=-1, keepdims=True))
    centered = values - average
    inverse = lax.rsqrt(lax.optimization_barrier(jnp.mean(centered * centered, axis=-1, keepdims=True)) + epsilon)
    return (centered * inverse, inverse)

def normalize_back(gradient, normed, inverse):
    mean_grad = lax.optimization_barrier(jnp.mean(gradient, axis=-1, keepdims=True))
    mean_both = lax.optimization_barrier(jnp.mean(gradient * normed, axis=-1, keepdims=True))
    return (gradient - mean_grad - normed * mean_both) * inverse

def narrow(values):
    return lax.optimization_barrier(values.astype(jnp.bfloat16)).astype(jnp.float32)

def reference(tokens, cotangent, qkv_weight, out_weight):
    all_columns = HEADS * HD
    score_scale = HD ** (-0.5)
    flat_weight = qkv_weight.reshape(D, 3 * all_columns)
    qkv_total = jnp.zeros((D, 3 * all_columns), jnp.float32)
    out_total = jnp.zeros((D, all_columns), jnp.float32)
    branches = []
    for batch_row in range(BATCH):
        row_grads = cotangent[batch_row]
        normed, inverse = normalize(tokens[batch_row].astype(jnp.float32))
        unit_low = normed.astype(jnp.bfloat16)
        projected = jnp.dot(unit_low, flat_weight, preferred_element_type=jnp.float32)
        query_unit, query_inv = normalize(projected[:, :all_columns].reshape(SEQ_LEN, HEADS, HD))
        key_unit, key_inv = normalize(projected[:, all_columns:2 * all_columns].reshape(SEQ_LEN, HEADS, HD))
        query_low = narrow(query_unit)
        key_low = narrow(key_unit)
        value_low = narrow(projected[:, 2 * all_columns:].reshape(SEQ_LEN, HEADS, HD))
        scores = jnp.einsum('qhd,khd->hqk', query_low, key_low) * score_scale
        exponent = jnp.exp(scores)
        exp_total = lax.optimization_barrier(jnp.sum(exponent, axis=-1))
        attended = jnp.einsum('hqk,khd->qhd', narrow(exponent), value_low) / exp_total.T[:, :, None]
        attended_low = attended.astype(jnp.bfloat16)
        attended_wide = lax.optimization_barrier(attended_low).astype(jnp.float32)
        grad_low = jnp.dot(row_grads, out_weight, preferred_element_type=jnp.float32).astype(jnp.bfloat16)
        grad_wide = lax.optimization_barrier(grad_low).astype(jnp.float32).reshape(SEQ_LEN, HEADS, HD)
        row_delta = lax.optimization_barrier(jnp.sum(grad_wide * attended_wide, axis=-1))
        probability = exponent / exp_total[:, :, None]
        prob_grad = jnp.einsum('qhd,khd->hqk', grad_wide, value_low)
        grad_score = narrow(probability * (prob_grad - row_delta.T[:, :, None]) * score_scale)
        query_raw = jnp.einsum('hqk,khd->qhd', grad_score, key_low)
        key_raw = jnp.einsum('hqk,qhd->khd', grad_score, query_low)
        value_raw = jnp.einsum('hqk,qhd->khd', narrow(probability), grad_wide)
        query_back = normalize_back(query_raw, query_unit, query_inv)
        key_back = normalize_back(key_raw, key_unit, key_inv)
        qkv_low = jnp.concatenate([query_back.reshape(SEQ_LEN, all_columns), key_back.reshape(SEQ_LEN, all_columns), value_raw.reshape(SEQ_LEN, all_columns)], axis=1).astype(jnp.bfloat16)
        inner_grad = jnp.dot(qkv_low, flat_weight.T, preferred_element_type=jnp.float32)
        branches.append(normalize_back(inner_grad, normed, inverse).astype(jnp.bfloat16))
        attended_flat = attended_low.reshape(SEQ_LEN, all_columns)
        for block_index in range(N_SEQ):
            low_row = block_index * TOK_DEV
            high_row = low_row + TOK_DEV
            qkv_total = qkv_total + narrow(jnp.dot(unit_low[low_row:high_row].T, qkv_low[low_row:high_row], preferred_element_type=jnp.float32))
            out_total = out_total + narrow(jnp.dot(row_grads[low_row:high_row].T, attended_flat[low_row:high_row], preferred_element_type=jnp.float32))
    return (qkv_total.reshape(D, 3, all_columns), out_total, jnp.stack(branches))
```

```python
import functools

import jax
import jax.numpy as jnp
from jax import lax
from jax.experimental import pallas as pl
from jax.experimental.pallas import tpu as pltpu
from jax.sharding import PartitionSpec as P

HD = 128
CORES = 2
MESH_ID = pl.DeviceIdType.MESH
EPSILON = 1e-06
F32, BF16 = jnp.float32, jnp.bfloat16


def dot(left, right):
    return jnp.dot(left, right, preferred_element_type=F32)


def dot_nt(left, right):
    return lax.dot_general(left, right, (((1,), (1,)), ((), ())), preferred_element_type=F32)


def dot_tn(left, right):
    return lax.dot_general(left, right, (((0,), (0,)), ((), ())), preferred_element_type=F32)


def normalize(values):
    centered = values - jnp.mean(values, axis=-1, keepdims=True)
    inverse = lax.rsqrt(jnp.mean(centered * centered, axis=-1, keepdims=True) + EPSILON)
    return centered * inverse, inverse


def normalize_back(gradient, normed, inverse):
    mean_grad = jnp.mean(gradient, axis=-1, keepdims=True)
    mean_both = jnp.mean(gradient * normed, axis=-1, keepdims=True)
    return (gradient - mean_grad - normed * mean_both) * inverse


def body(
    sizes,
    tokens_hbm,
    cotangent_hbm,
    qkv_hbm,
    outw_hbm,
    qkv_out,
    outw_out,
    branch_out,
    tok,
    cot,
    unit_low,
    unit_t,
    cot_t,
    stat_mean,
    stat_inv,
    w_kv,
    w_qo,
    acc_kv,
    acc_qo,
    pairs,
    query_low,
    query_unit,
    key_unit,
    query_inv,
    key_inv,
    grad_low,
    expo,
    totals,
    deltas,
    weighted,
    attended,
    query_raw,
    part,
    part_in,
    back_q,
    back_kv,
    inner,
    inner_in,
    sums,
    sums_in,
    term_kv,
    term_qo,
    core_kv,
    core_qo,
    chip_kv,
    chip_qo,
    chain_kv,
    chain_qo,
    load_sem,
    w_recv,
    w_right,
    w_left,
    w_chip,
    w_core,
    p_recv,
    p_right,
    p_left,
    g_low,
    g_high,
    g_send,
    t_core_send,
    t_core_recv,
    t_chip_send,
    t_chip_recv,
    t_chain_send,
    t_low_recv,
    t_high_recv,
    x_send,
    x_recv,
    xs_send,
    xs_recv,
):
    seq_count, dp_count, tensor_count, own_rows, head_count = sizes
    chip_count = dp_count // CORES
    token_count, feature_count = tok.shape
    columns = head_count * HD
    share = feature_count // tensor_count
    plane = dp_count * own_rows
    scale = HD ** (-0.5)
    place = lax.axis_index("seq")
    index = lax.axis_index("dp")
    lane = lax.axis_index("tensor")
    chip, core = index // CORES, index % CORES
    not_last, not_first = place < seq_count - 1, place > 0
    weights, terms = (w_kv, w_qo), (term_kv, term_qo)
    held, chip_in = (core_kv, core_qo), (chip_kv, chip_qo)
    chain_in = (chain_kv, chain_qo)
    KV, QO = 0, 1

    own_slot = place * dp_count + index

    def rows_of(slot):
        return pl.ds(pl.multiple_of(slot * own_rows, own_rows), own_rows)

    loads = [
        pltpu.make_async_copy(
            qkv_hbm.at[pl.ds(1, 2)], w_kv.at[:, rows_of(own_slot), :], load_sem.at[0]
        ),
        pltpu.make_async_copy(qkv_hbm.at[0], w_qo.at[0, rows_of(own_slot), :], load_sem.at[1]),
        pltpu.make_async_copy(outw_hbm, w_qo.at[1, rows_of(own_slot), :], load_sem.at[2]),
        pltpu.make_async_copy(tokens_hbm, tok, load_sem.at[3]),
        pltpu.make_async_copy(cotangent_hbm, cot, load_sem.at[4]),
    ]
    for load in loads:
        load.start()

    barrier = pltpu.get_barrier_semaphore()

    def signal(device):
        pl.semaphore_signal(barrier, inc=1, device_id=device, device_id_type=MESH_ID)

    @pl.when(not_first)
    def _():
        signal({"seq": place - 1})

    @pl.when(not_last)
    def _():
        signal({"seq": place + 1})

    for step in range(1, chip_count):
        signal({"dp": (chip + step) % chip_count * CORES + core})
    signal({"dp": chip * CORES + 1 - core})
    for step in range(1, tensor_count):
        signal({"tensor": (lane + step) % tensor_count})
    ends = jnp.minimum(place, 1) + jnp.minimum(seq_count - 1 - place, 1)
    pl.semaphore_wait(barrier, chip_count + tensor_count - 1 + ends)

    def remote(source, target, send_sem, recv_sem, device):
        return pltpu.make_async_remote_copy(
            src_ref=source,
            dst_ref=target,
            send_sem=send_sem,
            recv_sem=recv_sem,
            device_id=device,
            device_id_type=MESH_ID,
        )

    up, down = {"seq": place + 1}, {"seq": place - 1}
    beside_device = {"dp": chip * CORES + 1 - core}

    def chip_device(step):
        return {"dp": (chip + step) % chip_count * CORES + core}

    both_sides = jnp.minimum(place, seq_count - 1 - place)

    def origin_at(k):
        if k == 0:
            return place
        near = place - (k + 1) // 2 if k % 2 else place + k // 2
        far = jnp.where(place * 2 > seq_count - 1, place - (k - both_sides), place + (k - both_sides))
        return jnp.where(k <= 2 * both_sides, near, far)

    def w_copy(half, slot, send_sem, device):
        ref = weights[half].at[:, rows_of(slot), :]
        return remote(ref, ref, send_sem, w_recv.at[half, slot], device)

    def w_side(half, origin, rightward):
        if rightward:
            return w_copy(half, origin * dp_count + index, w_right.at[half, origin], up)
        return w_copy(half, origin * dp_count + index, w_left.at[half, origin], down)

    def w_across(half, origin, step):
        sem = w_chip.at[half, origin * chip_count + step]
        return w_copy(half, origin * dp_count + index, sem, chip_device(step))

    def w_beside(half, origin, source_chip):
        sem = w_core.at[half, origin * chip_count + source_chip]
        return w_copy(half, origin * dp_count + source_chip * CORES + core, sem, beside_device)

    def w_landed(half, slot):
        w_copy(half, slot, w_core.at[half, 0], beside_device).wait_recv()

    def w_sides_own(half):
        @pl.when(not_last)
        def _():
            w_side(half, place, True).start()

        @pl.when(not_first)
        def _():
            w_side(half, place, False).start()

    def w_spread(half, origin):
        for step in range(1, chip_count):
            w_across(half, origin, step).start()

    def w_step(half, k):
        origin = origin_at(k)
        w_landed(half, origin * dp_count + index)

        @pl.when((origin < place) & not_last)
        def _():
            w_side(half, origin, True).start()

        @pl.when((origin > place) & not_first)
        def _():
            w_side(half, origin, False).start()

        w_spread(half, origin)
        w_beside(half, origin, chip).start()

    def w_chip_step(half, k):
        origin = origin_at(k)
        for step in range(1, chip_count):
            source_chip = (chip + step) % chip_count
            w_landed(half, origin * dp_count + source_chip * CORES + core)
            w_beside(half, origin, source_chip).start()

    def project(half, k):
        origin = origin_at(k)
        for source_chip in range(chip_count):
            w_landed(half, origin * dp_count + source_chip * CORES + 1 - core)
        rows = pl.ds(pl.multiple_of(origin * plane, plane), plane)
        acc = (acc_kv, acc_qo)[half]
        for j in range(2):
            source = cot if (half == QO and j == 1) else unit_low
            product = dot(source[:, rows], weights[half][j, rows, :])
            if k == 0:
                acc[j] = product
            else:
                acc[j] += product

    def block_rows(origin):
        return pl.ds(pl.multiple_of(origin * token_count, token_count), token_count)

    def p_copy(origin, rightward):
        ref = pairs.at[:, block_rows(origin), :]
        if rightward:
            return remote(ref, ref, p_right.at[origin], p_recv.at[origin], up)
        return remote(ref, ref, p_left.at[origin], p_recv.at[origin], down)

    def p_step(k):
        origin = origin_at(k)
        p_copy(origin, True).wait_recv()

        @pl.when((origin < place) & not_last)
        def _():
            p_copy(origin, True).start()

        @pl.when((origin > place) & not_first)
        def _():
            p_copy(origin, False).start()

    loads[0].wait()
    w_sides_own(KV)
    w_spread(KV, place)
    w_beside(KV, place, chip).start()
    loads[1].wait()
    loads[2].wait()
    loads[3].wait()
    loads[4].wait()

    @pl.loop(0, token_count // 32)
    def _(step):
        rows = pl.ds(pl.multiple_of(step * 32, 32), 32)
        values = tok[rows, :].astype(F32)
        average = jnp.mean(values, axis=-1, keepdims=True)
        centered = values - average
        inverse = lax.rsqrt(jnp.mean(centered * centered, axis=-1, keepdims=True) + EPSILON)
        unit_low[rows, :] = (centered * inverse).astype(BF16)
        stat_mean[rows, :] = jnp.broadcast_to(average, (32, 128))
        stat_inv[rows, :] = jnp.broadcast_to(inverse, (32, 128))

    def flip(source, target):
        @pl.loop(0, feature_count // 128)
        def _(step):
            cut = pl.ds(pl.multiple_of(step * 128, 128), 128)
            target[cut, :] = source[:, cut].T

    fill = [lambda: flip(unit_low, unit_t), lambda: flip(cot, cot_t)]
    own_qo_at = min(2, seq_count - 1)
    for k in range(1, seq_count):
        w_step(KV, k)
        if k == own_qo_at:
            w_sides_own(QO)
            w_beside(QO, place, chip).start()
        if k == seq_count - 1:
            w_spread(QO, place)
        w_chip_step(KV, k - 1)
        project(KV, k - 1)
        if fill:
            fill.pop(0)()
    for rest in fill:
        rest()
    w_chip_step(KV, seq_count - 1)
    project(KV, seq_count - 1)

    own_block = block_rows(place)
    for h in range(head_count):
        cut = slice(h * HD, (h + 1) * HD)
        normed, inverse = normalize(acc_kv[0, :, cut])
        key_unit[:, cut] = normed
        key_inv[:, cut] = jnp.broadcast_to(inverse, (token_count, HD))
        pairs[0, own_block, cut] = normed.astype(BF16)
        pairs[1, own_block, cut] = acc_kv[1, :, cut].astype(BF16)

    for k in range(1, min(3, seq_count)):
        w_step(QO, k)

    @pl.when(not_last)
    def _():
        p_copy(place, True).start()

    @pl.when(not_first)
    def _():
        p_copy(place, False).start()

    w_chip_step(QO, 0)
    project(QO, 0)
    for k in range(3, seq_count):
        w_step(QO, k)
    for k in range(1, seq_count - 1):
        w_chip_step(QO, k)
        project(QO, k)
    if seq_count > 1:
        p_step(1)
    if seq_count > 1:
        w_chip_step(QO, seq_count - 1)
        project(QO, seq_count - 1)
    for h in range(head_count):
        cut = slice(h * HD, (h + 1) * HD)
        normed, inverse = normalize(acc_qo[0, :, cut])
        query_unit[:, cut] = normed
        query_inv[:, cut] = jnp.broadcast_to(inverse, (token_count, HD))
        query_low[:, cut] = normed.astype(BF16)
    grad_low[...] = acc_qo[1].astype(BF16)

    def head_cut(h):
        return pl.ds(pl.multiple_of(h * HD, HD), HD)

    def expo_at(origin, h):
        row = (h * seq_count + origin) * token_count
        return pl.ds(pl.multiple_of(row, token_count), token_count)

    def attend(k):
        origin = origin_at(k)

        @pl.loop(0, head_count)
        def _(h):
            cut = head_cut(h)
            rows = block_rows(origin)
            scores = dot_nt(query_low[:, cut], pairs[0, rows, cut]) * scale
            exponent = jnp.exp(scores)
            low = exponent.astype(BF16)
            expo[expo_at(origin, h), :] = low
            total = exponent[:, :HD]
            for at in range(HD, token_count, HD):
                total = total + exponent[:, at : at + HD]
            mixed = dot(low, pairs[1, rows, cut])
            if k == 0:
                totals[h] = total
                weighted[:, cut] = mixed
            else:
                totals[h] += total
                weighted[:, cut] += mixed

    attend(0)
    for k in range(1, seq_count):
        if k > 1:
            p_step(k)
        attend(k)
    for h in range(head_count):
        cut = slice(h * HD, (h + 1) * HD)
        total = jnp.sum(totals[h], axis=-1, keepdims=True)
        low = (weighted[:, cut] / total).astype(BF16)
        attended[:, cut] = low
        both = grad_low[:, cut].astype(F32) * low.astype(F32)
        totals[h] = jnp.broadcast_to(1.0 / total, (token_count, HD))
        deltas[h] = jnp.broadcast_to(jnp.sum(both, axis=-1, keepdims=True), (token_count, HD))

    order = []
    for turn in range((seq_count + 1) // 2):
        order.extend(sorted({seq_count - 1 - turn, turn}, reverse=True))
    mirror = jnp.where(place * 2 < seq_count, 0, 1)

    def target_at(n):
        return order[n] + mirror * (seq_count - 1 - 2 * order[n])

    def from_above(target, receiver):
        return jnp.where(target == receiver, seq_count, target)

    def g_copy(target, rightward):
        rows = block_rows(target)
        source = part.at[:, rows, :]
        if rightward:
            into, sem, device = rows, g_low, up
        else:
            into, sem, device = block_rows(from_above(target, place - 1)), g_high, down
        return remote(source, part_in.at[:, into, :], g_send.at[target], sem.at[target], device)

    def backward(n):
        target = target_at(n)

        @pl.loop(0, head_count)
        def _(h):
            cut = head_cut(h)
            rows = block_rows(target)
            inv_total = totals[h][:, :1]
            probability = expo[expo_at(target, h), :].astype(F32) * inv_total
            gradient = grad_low[:, cut]
            prob_grad = dot_nt(gradient, pairs[1, rows, cut])
            score = (probability * (prob_grad - deltas[h][:, :1]) * scale).astype(BF16)
            query_part = dot(score, pairs[0, rows, cut])
            part[0, rows, cut] = dot_tn(score, query_low[:, cut]).astype(BF16)
            part[1, rows, cut] = dot_tn(probability.astype(BF16), gradient).astype(BF16)
            if n == 0:
                query_raw[:, cut] = query_part
            else:
                query_raw[:, cut] += query_part

    for n in range(seq_count):
        backward(n)
        target = target_at(n)

        @pl.when((target > place) & (place == 0))
        def _():
            g_copy(target, True).start()

        @pl.when((target < place) & (place == seq_count - 1))
        def _():
            g_copy(target, False).start()

    for h in range(head_count):
        cut = slice(h * HD, (h + 1) * HD)
        raised = normalize_back(query_raw[:, cut], query_unit[:, cut], query_inv[:, cut])
        back_q[:, cut] = raised.astype(BF16)

    def t_piece(ref, slot):
        return ref.at[:, rows_of(slot), :]

    def t_beside(half, target, target_chip):
        slot = target * chip_count + target_chip
        source = t_piece(terms[half], target * dp_count + target_chip * CORES + 1 - core)
        into = t_piece(held[half], slot)
        sems = t_core_send.at[half, slot], t_core_recv.at[half, slot]
        return remote(source, into, *sems, beside_device)

    def t_across(half, target, step):
        other = (chip + step) % chip_count
        slot = (step - 1) * seq_count + target
        source = t_piece(held[half], target * chip_count + other)
        into = t_piece(chip_in[half], slot)
        sems = t_chip_send.at[half, slot], t_chip_recv.at[half, slot]
        return remote(source, into, *sems, chip_device(step))

    def t_chain(half, target, rightward):
        source = t_piece(held[half], target * chip_count + chip)
        if rightward:
            at, sem, device = target, t_low_recv, up
        else:
            at, sem, device = from_above(target, place - 1), t_high_recv, down
        send_sem = t_chain_send.at[half, target]
        into = t_piece(chain_in[half], at)
        return remote(source, into, send_sem, sem.at[half, target], device)

    def add_into(ref, slot, others, size):
        @pl.loop(0, size // 16)
        def _(step):
            def cut(at):
                return pl.ds(pl.multiple_of(at * size + step * 16, 16), 16)

            for j in range(2):
                total = ref[j, cut(slot), :].astype(F32)
                for other, at in others:
                    total = total + other[j, cut(at), :].astype(F32)
                ref[j, cut(slot), :] = total.astype(BF16)

    def make_terms(half, n):
        target = target_at(n)

        @pl.loop(0, dp_count)
        def _(at):
            rows = rows_of(target * dp_count + at)
            for j in range(2):
                if half == KV:
                    product = dot(unit_t[rows, :], back_kv[j])
                elif j == 0:
                    product = dot(unit_t[rows, :], back_q[...])
                else:
                    product = dot(cot_t[rows, :], attended[...])
                terms[half][j, rows, :] = product.astype(BF16)

        for step in range(1, chip_count):
            t_beside(half, target, (chip + step) % chip_count).start()
        t_beside(half, target, chip).start()

    def send_across(half, n):
        target = target_at(n)
        for step in range(1, chip_count):
            other = (chip + step) % chip_count
            t_beside(half, target, other).wait_recv()
            slot = target * chip_count + other
            add_into(
                held[half], slot, [(terms[half], target * dp_count + other * CORES + core)], own_rows
            )
            t_across(half, target, step).start()

    def chain(half, n):
        target = target_at(n)
        slot = target * chip_count + chip
        t_beside(half, target, chip).wait_recv()
        others = [(terms[half], target * dp_count + index)]
        for step in range(1, chip_count):
            t_across(half, target, step).wait_recv()
            others.append((chip_in[half], (step - 1) * seq_count + target))
        add_into(held[half], slot, others, own_rows)

        @pl.when(place < target)
        def _():
            @pl.when(not_first)
            def _():
                t_chain(half, target, True).wait_recv()
                add_into(held[half], slot, [(chain_in[half], target)], own_rows)

            t_chain(half, target, True).start()

        @pl.when(place > target)
        def _():
            @pl.when(not_last)
            def _():
                t_chain(half, target, False).wait_recv()
                add_into(held[half], slot, [(chain_in[half], target)], own_rows)

            t_chain(half, target, False).start()

    for n in range(seq_count):
        make_terms(QO, n)
    for n in range(seq_count):
        send_across(QO, n)

    for n in range(seq_count):
        target = target_at(n)

        @pl.when((place < target) & not_first)
        def _():
            g_copy(target, True).wait_recv()
            add_into(part, target, [(part_in, target)], token_count)
            g_copy(target, True).start()

        @pl.when((place > target) & not_last)
        def _():
            g_copy(target, False).wait_recv()
            add_into(part, target, [(part_in, target)], token_count)
            g_copy(target, False).start()

    @pl.when(not_first)
    def _():
        g_copy(place, True).wait_recv()
        add_into(part, place, [(part_in, place)], token_count)

    @pl.when(not_last)
    def _():
        g_copy(place, False).wait_recv()
        add_into(part, place, [(part_in, seq_count)], token_count)

    for h in range(head_count):
        cut = slice(h * HD, (h + 1) * HD)
        raw = part[0, own_block, cut].astype(F32)
        raised = normalize_back(raw, key_unit[:, cut], key_inv[:, cut])
        back_kv[0, :, cut] = raised.astype(BF16)
        back_kv[1, :, cut] = part[1, own_block, cut]

    for n in range(seq_count):
        make_terms(KV, n)
    for n in range(seq_count):
        send_across(KV, n)

    width = next(size for size in (512, 384, 256, 128) if share % size == 0)
    sums[...] = jnp.zeros_like(sums)

    def lanes(values):
        total = values[:, :128]
        for at in range(128, width, 128):
            total = total + values[:, at : at + 128]
        return total

    @pl.loop(0, feature_count // width)
    def _(step):
        cut = pl.ds(pl.multiple_of(step * width, width), width)
        product = dot_nt(back_q[...], w_qo[0, cut, :])
        product = product + dot_nt(back_kv[0], w_kv[0, cut, :])
        product = product + dot_nt(back_kv[1], w_kv[1, cut, :])
        unit = (tok[:, cut].astype(F32) - stat_mean[:, :1]) * stat_inv[:, :1]
        sums[0] += lanes(product)
        sums[1] += lanes(product * unit)
        inner[step // (share // width), :, pl.ds(
            pl.multiple_of(step % (share // width) * width, width), width
        )] = product.astype(BF16)

    def x_copy(step):
        other = (lane + step) % tensor_count
        return remote(
            inner.at[other],
            inner_in.at[step - 1],
            x_send.at[step - 1],
            x_recv.at[step - 1],
            {"tensor": other},
        )

    def xs_copy(step):
        other = (lane + step) % tensor_count
        return remote(
            sums,
            sums_in.at[step - 1],
            xs_send.at[step - 1],
            xs_recv.at[step - 1],
            {"tensor": other},
        )

    for step in range(1, tensor_count):
        x_copy(step).start()
        xs_copy(step).start()
    for n in range(seq_count):
        chain(QO, n)

    def finish_branch():
        for step in range(1, tensor_count):
            x_copy(step).wait_recv()
            xs_copy(step).wait_recv()

        @pl.loop(0, token_count // 16)
        def _(step):
            rows = pl.ds(pl.multiple_of(step * 16, 16), 16)
            first, second = sums[0, rows, :], sums[1, rows, :]
            values = inner[lane, rows, :].astype(F32)
            for other in range(tensor_count - 1):
                first = first + sums_in[other, 0, rows, :]
                second = second + sums_in[other, 1, rows, :]
                values = values + inner_in[other, rows, :].astype(F32)
            mean_grad = jnp.sum(first, axis=-1, keepdims=True) / feature_count
            mean_both = jnp.sum(second, axis=-1, keepdims=True) / feature_count
            cut = pl.ds(pl.multiple_of(lane * share, share), share)
            inverse = stat_inv[rows, :][:, :1]
            unit = (tok[rows, cut].astype(F32) - stat_mean[rows, :][:, :1]) * inverse
            branch_out[rows, :] = ((values - mean_grad - unit * mean_both) * inverse).astype(BF16)

    for n in range(seq_count):
        chain(KV, n)
    finish_branch()

    own_held = place * chip_count + chip
    for half in (QO, KV):

        @pl.when(not_first)
        def _():
            t_chain(half, place, True).wait_recv()

        @pl.when(not_last)
        def _():
            t_chain(half, place, False).wait_recv()

        @pl.loop(0, own_rows // 16)
        def _(step):
            rows = pl.ds(pl.multiple_of(step * 16, 16), 16)

            def cut(at):
                return pl.ds(pl.multiple_of(at * own_rows + step * 16, 16), 16)

            for j in range(2):
                if half == KV:
                    target = qkv_out.at[1 + j]
                else:
                    target = outw_out if j else qkv_out.at[0]
                target[rows, :] = held[half][j, cut(own_held), :].astype(F32)

                @pl.when(not_first)
                def _():
                    target[rows, :] += chain_in[half][j, cut(place), :].astype(F32)

                @pl.when(not_last)
                def _():
                    target[rows, :] += chain_in[half][j, cut(seq_count), :].astype(F32)

    for origin in range(seq_count):
        to_right = (origin <= place) & not_last
        to_left = (origin >= place) & not_first
        for half in (KV, QO):
            for step in range(1, chip_count):
                w_across(half, origin, step).wait_send()
                t_across(half, origin, step).wait_send()
            for source_chip in range(chip_count):
                w_beside(half, origin, source_chip).wait_send()
                t_beside(half, origin, source_chip).wait_send()

            @pl.when(to_right)
            def _():
                w_side(half, origin, True).wait_send()

            @pl.when(to_left)
            def _():
                w_side(half, origin, False).wait_send()

            @pl.when(place != origin)
            def _():
                t_chain(half, origin, True).wait_send()

        @pl.when(to_right)
        def _():
            p_copy(origin, True).wait_send()

        @pl.when(to_left)
        def _():
            p_copy(origin, False).wait_send()

        @pl.when(place != origin)
        def _():
            g_copy(origin, True).wait_send()

    for step in range(1, tensor_count):
        x_copy(step).wait_send()
        xs_copy(step).wait_send()


def local(tokens, cotangent, qkv_weight, out_weight):
    seq_count, dp_count = lax.axis_size("seq"), lax.axis_size("dp")
    tensor_count = lax.axis_size("tensor")
    chip_count = dp_count // CORES
    row_count, feature_count = tokens.shape[1:]
    own_rows, columns = out_weight.shape
    head_count = columns // HD
    share = feature_count // tensor_count
    sizes = (seq_count, dp_count, tensor_count, own_rows, head_count)

    def vmem(*shape, kind=BF16):
        return pltpu.VMEM(shape, kind)

    def dma(*shape):
        return pltpu.SemaphoreType.DMA(shape)

    both, peers = seq_count * chip_count, seq_count * (chip_count - 1)
    scratch = [
        vmem(row_count, feature_count),
        vmem(row_count, feature_count),
        vmem(row_count, feature_count),
        vmem(feature_count, row_count),
        vmem(feature_count, row_count),
        vmem(row_count, 128, kind=F32),
        vmem(row_count, 128, kind=F32),
        vmem(2, feature_count, columns),
        vmem(2, feature_count, columns),
        vmem(2, row_count, columns, kind=F32),
        vmem(2, row_count, columns, kind=F32),
        vmem(2, seq_count * row_count, columns),
        vmem(row_count, columns),
        vmem(row_count, columns, kind=F32),
        vmem(row_count, columns, kind=F32),
        vmem(row_count, columns, kind=F32),
        vmem(row_count, columns, kind=F32),
        vmem(row_count, columns),
        vmem(head_count * seq_count * row_count, row_count),
        vmem(head_count, row_count, HD, kind=F32),
        vmem(head_count, row_count, HD, kind=F32),
        vmem(row_count, columns, kind=F32),
        vmem(row_count, columns),
        vmem(row_count, columns, kind=F32),
        vmem(2, seq_count * row_count, columns),
        vmem(2, (seq_count + 1) * row_count, columns),
        vmem(row_count, columns),
        vmem(2, row_count, columns),
        vmem(tensor_count, row_count, share),
        vmem(max(tensor_count - 1, 1), row_count, share),
        vmem(2, row_count, 128, kind=F32),
        vmem(max(tensor_count - 1, 1), 2, row_count, 128, kind=F32),
        vmem(2, feature_count, columns),
        vmem(2, feature_count, columns),
        vmem(2, both * own_rows, columns),
        vmem(2, both * own_rows, columns),
        vmem(2, max(peers, 1) * own_rows, columns),
        vmem(2, max(peers, 1) * own_rows, columns),
        vmem(2, (seq_count + 1) * own_rows, columns),
        vmem(2, (seq_count + 1) * own_rows, columns),
        dma(5),
        dma(2, seq_count * dp_count),
        dma(2, seq_count),
        dma(2, seq_count),
        dma(2, both),
        dma(2, both),
        dma(seq_count),
        dma(seq_count),
        dma(seq_count),
        dma(seq_count),
        dma(seq_count),
        dma(seq_count),
        dma(2, both),
        dma(2, both),
        dma(2, max(peers, 1)),
        dma(2, max(peers, 1)),
        dma(2, seq_count),
        dma(2, seq_count),
        dma(2, seq_count),
        dma(max(tensor_count - 1, 1)),
        dma(max(tensor_count - 1, 1)),
        dma(max(tensor_count - 1, 1)),
        dma(max(tensor_count - 1, 1)),
    ]
    anywhere = pl.BlockSpec(memory_space=pl.ANY)
    vector = pl.BlockSpec(memory_space=pltpu.VMEM)
    qkv_grad, out_grad, branch = pl.pallas_call(
        functools.partial(body, sizes),
        out_shape=(
            jax.ShapeDtypeStruct((3, own_rows, columns), F32),
            jax.ShapeDtypeStruct((own_rows, columns), F32),
            jax.ShapeDtypeStruct((row_count, share), BF16),
        ),
        in_specs=[anywhere] * 4,
        out_specs=(vector, vector, vector),
        scratch_shapes=scratch,
        compiler_params=pltpu.CompilerParams(
            collective_id=0, has_side_effects=True, vmem_limit_bytes=67043328
        ),
        name="layer",
    )(tokens[0], cotangent[0], jnp.transpose(qkv_weight, (1, 0, 2)), out_weight)
    return jnp.transpose(qkv_grad, (1, 0, 2)), out_grad, branch[None]


def solution(mesh):
    return jax.shard_map(
        local,
        mesh=mesh,
        in_specs=(
            P("dp", "seq", None),
            P("dp", "seq", None),
            P(("seq", "dp"), None, "tensor"),
            P(("seq", "dp"), "tensor"),
        ),
        out_specs=(
            P(("seq", "dp"), None, "tensor"),
            P(("seq", "dp"), "tensor"),
            P("dp", "seq", "tensor"),
        ),
        check_vma=False,
    )
```

```python
import functools

import jax
import jax.numpy as jnp
from jax import lax
from jax.experimental import pallas as pl
from jax.experimental.pallas import tpu as pltpu
from jax.sharding import PartitionSpec as P

HD = 128
CORES = 2
MESH_ID = pl.DeviceIdType.MESH
EPSILON = 1e-06
F32, BF16 = jnp.float32, jnp.bfloat16


def dot(left, right):
    return jnp.dot(left, right, preferred_element_type=F32)


def dot_nt(left, right):
    return lax.dot_general(left, right, (((1,), (1,)), ((), ())), preferred_element_type=F32)


def dot_tn(left, right):
    return lax.dot_general(left, right, (((0,), (0,)), ((), ())), preferred_element_type=F32)


def normalize(values):
    centered = values - jnp.mean(values, axis=-1, keepdims=True)
    inverse = lax.rsqrt(jnp.mean(centered * centered, axis=-1, keepdims=True) + EPSILON)
    return centered * inverse, inverse


def normalize_back(gradient, normed, inverse):
    mean_grad = jnp.mean(gradient, axis=-1, keepdims=True)
    mean_both = jnp.mean(gradient * normed, axis=-1, keepdims=True)
    return (gradient - mean_grad - normed * mean_both) * inverse


def body(
    sizes,
    tokens_hbm,
    cotangent_hbm,
    qkv_hbm,
    outw_hbm,
    qkv_out,
    outw_out,
    branch_hbm,
    tok,
    cot,
    unit_low,
    unit_t,
    cot_t,
    stat_mean,
    stat_inv,
    weights,
    acc,
    pairs,
    query_low,
    query_unit,
    key_unit,
    query_inv,
    key_inv,
    grad_low,
    expo,
    totals,
    deltas,
    weighted,
    attended,
    query_raw,
    part,
    part_in,
    back,
    inner,
    inner_in,
    sums,
    terms,
    held,
    chip_in,
    chain_in,
    summed,
    branch_out,
    sum_rows,
    sum_rows_in,
    sum_columns,
    load_sem,
    store_sem,
    w_recv,
    w_right,
    w_left,
    w_chip,
    w_core,
    p_recv,
    p_right,
    p_left,
    g_low,
    g_high,
    g_send,
    t_core_send,
    t_core_recv,
    t_chip_send,
    t_chip_recv,
    t_chain_send,
    t_low_recv,
    t_high_recv,
    x_send,
    x_recv,
    xs_send,
    xs_recv,
):
    seq_count, dp_count, tensor_count, own_rows, head_count = sizes
    chip_count = dp_count // CORES
    token_count, feature_count = tok.shape
    share = feature_count // tensor_count
    plane = dp_count * own_rows
    scale = HD ** (-0.5)
    place = lax.axis_index("seq")
    index = lax.axis_index("dp")
    lane = lax.axis_index("tensor")
    chip, core = index // CORES, index % CORES
    not_last, not_first = place < seq_count - 1, place > 0
    both_sides = jnp.minimum(place, seq_count - 1 - place)
    KEY, VALUE, QUERY, OUT = range(4)

    def rows_of(slot):
        return pl.ds(pl.multiple_of(slot * own_rows, own_rows), own_rows)

    def block_rows(origin):
        return pl.ds(pl.multiple_of(origin * token_count, token_count), token_count)

    own_rows_at = rows_of(place * dp_count + index)
    loads = [
        pltpu.make_async_copy(
            qkv_hbm.at[pl.ds(1, 2)], weights.at[pl.ds(0, 2), own_rows_at, :], load_sem.at[0]
        ),
        pltpu.make_async_copy(qkv_hbm.at[0], weights.at[QUERY, own_rows_at, :], load_sem.at[1]),
        pltpu.make_async_copy(outw_hbm, weights.at[OUT, own_rows_at, :], load_sem.at[2]),
        pltpu.make_async_copy(tokens_hbm, tok, load_sem.at[3]),
        pltpu.make_async_copy(cotangent_hbm, cot, load_sem.at[4]),
    ]
    for load in loads:
        load.start()

    barrier = pltpu.get_barrier_semaphore()

    def signal(device):
        pl.semaphore_signal(barrier, inc=1, device_id=device, device_id_type=MESH_ID)

    def greet():
        @pl.when(not_first)
        def _():
            signal({"seq": place - 1})

        @pl.when(not_last)
        def _():
            signal({"seq": place + 1})

        for step in range(1, chip_count):
            signal({"dp": (chip + step) % chip_count * CORES + core})
        signal({"dp": chip * CORES + 1 - core})
        for step in range(1, tensor_count):
            signal({"tensor": (lane + step) % tensor_count})
        ends = jnp.minimum(place, 1) + jnp.minimum(seq_count - 1 - place, 1)
        pl.semaphore_wait(barrier, chip_count + tensor_count - 1 + ends)

    greet()

    def remote(source, target, send_sem, recv_sem, device):
        return pltpu.make_async_remote_copy(
            src_ref=source,
            dst_ref=target,
            send_sem=send_sem,
            recv_sem=recv_sem,
            device_id=device,
            device_id_type=MESH_ID,
        )

    up, down = {"seq": place + 1}, {"seq": place - 1}
    beside_device = {"dp": chip * CORES + 1 - core}

    def chip_device(step):
        return {"dp": (chip + step) % chip_count * CORES + core}

    def origin_at(k):
        near = jnp.where(k % 2 == 1, place - (k + 1) // 2, place + k // 2)
        far = jnp.where(
            place * 2 > seq_count - 1, place - (k - both_sides), place + (k - both_sides)
        )
        return jnp.where(k <= 2 * both_sides, near, far)

    event_count = 2 * (seq_count - 1)

    def event(number):
        group, rest = number // 4, number % 4
        if 2 * group + 2 <= seq_count - 1:
            paired = both_sides > group
            piece = jnp.where(paired, rest // 2, rest % 2)
            k = 2 * group + 1 + jnp.where(paired, rest % 2, rest // 2)
        else:
            piece, k = rest % 2, 2 * group + 1 + rest // 2
        return piece, origin_at(k)

    def events_until(k):
        return min(event_count, 4 * ((k + 1) // 2))

    def w_copy(piece, slot, send_sem, device):
        ref = weights.at[piece, rows_of(slot), :]
        return remote(ref, ref, send_sem, w_recv.at[piece, slot], device)

    def w_side(piece, origin, rightward):
        if rightward:
            return w_copy(piece, origin * dp_count + index, w_right.at[piece, origin], up)
        return w_copy(piece, origin * dp_count + index, w_left.at[piece, origin], down)

    def w_across(piece, origin, step):
        sem = w_chip.at[piece, origin * chip_count + step]
        return w_copy(piece, origin * dp_count + index, sem, chip_device(step))

    def w_beside(piece, origin, source_chip):
        sem = w_core.at[piece, origin * chip_count + source_chip]
        return w_copy(piece, origin * dp_count + source_chip * CORES + core, sem, beside_device)

    def w_landed(piece, slot):
        w_copy(piece, slot, w_core.at[piece, 0], beside_device).wait_recv()

    def w_sides_own(first):
        for piece in (first, first + 1):

            @pl.when(not_last)
            def _():
                w_side(piece, place, True).start()

            @pl.when(not_first)
            def _():
                w_side(piece, place, False).start()

    def w_spread_own(first):
        for piece in (first, first + 1):
            for step in range(1, chip_count):
                w_across(piece, place, step).start()
        for piece in (first, first + 1):
            w_beside(piece, place, chip).start()

    def w_step(first, number):
        piece, origin = event(number)
        piece = piece + first
        w_landed(piece, origin * dp_count + index)

        @pl.when((origin < place) & not_last)
        def _():
            w_side(piece, origin, True).start()

        @pl.when((origin > place) & not_first)
        def _():
            w_side(piece, origin, False).start()

        for step in range(1, chip_count):
            w_across(piece, origin, step).start()
        w_beside(piece, origin, chip).start()

    def w_chip_step(first, number):
        piece, origin = (number, place) if number < 2 else event(number - 2)
        piece = piece + first
        for step in range(1, chip_count):
            source_chip = (chip + step) % chip_count
            w_landed(piece, origin * dp_count + source_chip * CORES + core)
            w_beside(piece, origin, source_chip).start()

    def project(first, k):
        origin = origin_at(k)
        rows = pl.ds(pl.multiple_of(origin * plane, plane), plane)
        for piece in (first, first + 1):
            for source_chip in range(chip_count):
                w_landed(piece, origin * dp_count + source_chip * CORES + 1 - core)
        for piece in (first, first + 1):
            source = cot if piece == OUT else unit_low
            product = dot(source[:, rows], weights[piece, rows, :])
            if k == 0:
                acc[piece] = product
            else:
                acc[piece] += product

    def p_copy(piece, origin, rightward):
        ref = pairs.at[piece, block_rows(origin), :]
        if rightward:
            return remote(ref, ref, p_right.at[piece, origin], p_recv.at[piece, origin], up)
        return remote(ref, ref, p_left.at[piece, origin], p_recv.at[piece, origin], down)

    def p_step(number):
        piece, origin = event(number)
        p_copy(piece, origin, True).wait_recv()

        @pl.when((origin < place) & not_last)
        def _():
            p_copy(piece, origin, True).start()

        @pl.when((origin > place) & not_first)
        def _():
            p_copy(piece, origin, False).start()

    def p_sides_own():
        for piece in range(2):

            @pl.when(not_last)
            def _():
                p_copy(piece, place, True).start()

            @pl.when(not_first)
            def _():
                p_copy(piece, place, False).start()

    def normalize_tokens():
        @pl.loop(0, token_count // 32)
        def _(step):
            rows = pl.ds(pl.multiple_of(step * 32, 32), 32)
            values = tok[rows, :].astype(F32)
            average = jnp.mean(values, axis=-1, keepdims=True)
            centered = values - average
            inverse = lax.rsqrt(jnp.mean(centered * centered, axis=-1, keepdims=True) + EPSILON)
            unit_low[rows, :] = (centered * inverse).astype(BF16)
            stat_mean[rows, :] = jnp.broadcast_to(average, (32, 128))
            stat_inv[rows, :] = jnp.broadcast_to(inverse, (32, 128))

    def flip(source, target):
        @pl.loop(0, feature_count // 128)
        def _(step):
            cut = pl.ds(pl.multiple_of(step * 128, 128), 128)
            target[cut, :] = source[:, cut].T

    def key_ready():
        own_block = block_rows(place)
        for h in range(head_count):
            cut = slice(h * HD, (h + 1) * HD)
            normed, inverse = normalize(acc[KEY, :, cut])
            key_unit[:, cut] = normed
            key_inv[:, cut] = jnp.broadcast_to(inverse, (token_count, HD))
            pairs[0, own_block, cut] = normed.astype(BF16)
            pairs[1, own_block, cut] = acc[VALUE, :, cut].astype(BF16)

    def query_ready():
        for h in range(head_count):
            cut = slice(h * HD, (h + 1) * HD)
            normed, inverse = normalize(acc[QUERY, :, cut])
            query_unit[:, cut] = normed
            query_inv[:, cut] = jnp.broadcast_to(inverse, (token_count, HD))
            query_low[:, cut] = normed.astype(BF16)
        grad_low[...] = acc[OUT].astype(BF16)

    loads[0].wait()
    w_sides_own(KEY)
    w_spread_own(KEY)
    for load in loads[1:]:
        load.wait()
    normalize_tokens()

    chip_events = event_count + 2
    at_end = both_sides == 0
    early = min(4, event_count) - 1
    done = 0
    for number in range(event_count):
        w_step(KEY, number)
        if number == early:

            @pl.when(at_end)
            def _():
                w_sides_own(QUERY)

        if number == event_count - 1:

            @pl.when(jnp.logical_not(at_end))
            def _():
                w_sides_own(QUERY)

            w_spread_own(QUERY)
        if number >= 2:
            w_chip_step(KEY, done)
            done += 1
    planes = 0
    passed = 0
    while done < chip_events:
        if chip_events - done <= 2 and passed < min(2, event_count):
            w_step(QUERY, passed)
            passed += 1
        w_chip_step(KEY, done)
        done += 1
        while planes < seq_count - 1 and 2 + events_until(planes) <= done:
            project(KEY, planes)
            planes += 1
    while planes < seq_count:
        project(KEY, planes)
        planes += 1
    key_ready()
    while passed < event_count:
        w_step(QUERY, passed)
        passed += 1
    p_sides_own()
    flip(unit_low, unit_t)
    flip(cot, cot_t)
    done, planes, moved = 0, 0, 0
    while done < chip_events:
        left = chip_events - done
        if left <= 3:
            for _ in range(2 if left == 2 else 1):
                if moved < event_count:
                    p_step(moved)
                    moved += 1
        w_chip_step(QUERY, done)
        done += 1
        while planes < seq_count and 2 + events_until(planes) <= done:
            project(QUERY, planes)
            planes += 1
    query_ready()

    def head_cut(h):
        return pl.ds(pl.multiple_of(h * HD, HD), HD)

    def expo_at(origin, h):
        row = (h * seq_count + origin) * token_count
        return pl.ds(pl.multiple_of(row, token_count), token_count)

    def attend(k):
        origin = origin_at(k)

        @pl.loop(0, head_count)
        def _(h):
            cut = head_cut(h)
            rows = block_rows(origin)
            scores = dot_nt(query_low[:, cut], pairs[0, rows, cut]) * scale
            exponent = jnp.exp(scores)
            low = exponent.astype(BF16)
            expo[expo_at(origin, h), :] = low
            total = exponent[:, :HD]
            for at in range(HD, token_count, HD):
                total = total + exponent[:, at : at + HD]
            mixed = dot(low, pairs[1, rows, cut])
            if k == 0:
                totals[h] = total
                weighted[:, cut] = mixed
            else:
                totals[h] += total
                weighted[:, cut] += mixed

    def attend_end():
        for h in range(head_count):
            cut = slice(h * HD, (h + 1) * HD)
            total = jnp.sum(totals[h], axis=-1, keepdims=True)
            low = (weighted[:, cut] / total).astype(BF16)
            attended[:, cut] = low
            both = grad_low[:, cut].astype(F32) * low.astype(F32)
            totals[h] = jnp.broadcast_to(1.0 / total, (token_count, HD))
            deltas[h] = jnp.broadcast_to(jnp.sum(both, axis=-1, keepdims=True), (token_count, HD))

    for k in range(seq_count):
        while moved < events_until(k):
            p_step(moved)
            moved += 1
        attend(k)
    attend_end()

    def target_at(n):
        return origin_at(seq_count - 1 - n)

    def from_above(target, receiver):
        return jnp.where(target == receiver, seq_count, target)

    def add_into(ref, piece, slot, others, size):
        @pl.loop(0, size // 16)
        def _(step):
            def cut(at):
                return pl.ds(pl.multiple_of(at * size + step * 16, 16), 16)

            total = ref[piece, cut(slot), :].astype(F32)
            for other, at in others:
                total = total + other[piece, cut(at), :].astype(F32)
            ref[piece, cut(slot), :] = total.astype(BF16)

    def g_copy(piece, target, rightward):
        rows = block_rows(target)
        source = part.at[piece, rows, :]
        if rightward:
            into, sem, device = rows, g_low, up
        else:
            into, sem, device = block_rows(from_above(target, place - 1)), g_high, down
        into = part_in.at[piece, into, :]
        return remote(source, into, g_send.at[piece, target], sem.at[piece, target], device)

    def backward(n):
        target = target_at(n)

        @pl.loop(0, head_count)
        def _(h):
            cut = head_cut(h)
            rows = block_rows(target)
            inv_total = totals[h][:, :1]
            probability = expo[expo_at(target, h), :].astype(F32) * inv_total
            gradient = grad_low[:, cut]
            prob_grad = dot_nt(gradient, pairs[1, rows, cut])
            score = (probability * (prob_grad - deltas[h][:, :1]) * scale).astype(BF16)
            query_part = dot(score, pairs[0, rows, cut])
            part[0, rows, cut] = dot_tn(score, query_low[:, cut]).astype(BF16)
            part[1, rows, cut] = dot_tn(probability.astype(BF16), gradient).astype(BF16)
            if n == 0:
                query_raw[:, cut] = query_part
            else:
                query_raw[:, cut] += query_part

    def g_first(piece, n):
        target = target_at(n)

        @pl.when((target > place) & (place == 0))
        def _():
            g_copy(piece, target, True).start()

        @pl.when((target < place) & (place == seq_count - 1))
        def _():
            g_copy(piece, target, False).start()

    def g_step(piece, n):
        target = target_at(n)

        @pl.when((place < target) & not_first)
        def _():
            g_copy(piece, target, True).wait_recv()
            add_into(part, piece, target, [(part_in, target)], token_count)
            g_copy(piece, target, True).start()

        @pl.when((place > target) & not_last)
        def _():
            g_copy(piece, target, False).wait_recv()
            add_into(part, piece, target, [(part_in, target)], token_count)
            g_copy(piece, target, False).start()

    def g_own(piece):
        @pl.when(not_first)
        def _():
            g_copy(piece, place, True).wait_recv()
            add_into(part, piece, place, [(part_in, place)], token_count)

        @pl.when(not_last)
        def _():
            g_copy(piece, place, False).wait_recv()
            add_into(part, piece, place, [(part_in, seq_count)], token_count)

    def back_query():
        for h in range(head_count):
            cut = slice(h * HD, (h + 1) * HD)
            raised = normalize_back(query_raw[:, cut], query_unit[:, cut], query_inv[:, cut])
            back[QUERY, :, cut] = raised.astype(BF16)

    def back_keys():
        own_block = block_rows(place)
        for h in range(head_count):
            cut = slice(h * HD, (h + 1) * HD)
            raw = part[0, own_block, cut].astype(F32)
            raised = normalize_back(raw, key_unit[:, cut], key_inv[:, cut])
            back[KEY, :, cut] = raised.astype(BF16)

    def back_values():
        back[VALUE] = part[1, block_rows(place), :]

    def t_beside(piece, target, target_chip):
        slot = target * chip_count + target_chip
        source = terms.at[piece, rows_of(target * dp_count + target_chip * CORES + 1 - core), :]
        into = held.at[piece, rows_of(slot), :]
        sems = t_core_send.at[piece, slot], t_core_recv.at[piece, slot]
        return remote(source, into, *sems, beside_device)

    def t_across(piece, target, step):
        other = (chip + step) % chip_count
        slot = (step - 1) * seq_count + target
        source = held.at[piece, rows_of(target * chip_count + other), :]
        into = chip_in.at[piece, rows_of(slot), :]
        sems = t_chip_send.at[piece, slot], t_chip_recv.at[piece, slot]
        return remote(source, into, *sems, chip_device(step))

    def t_chain(piece, target, rightward):
        source = held.at[piece, rows_of(target * chip_count + chip), :]
        if rightward:
            at, sem, device = target, t_low_recv, up
        else:
            at, sem, device = from_above(target, place - 1), t_high_recv, down
        into = chain_in.at[piece, rows_of(at), :]
        return remote(source, into, t_chain_send.at[piece, target], sem.at[piece, target], device)

    def make_terms(piece, n):
        target = target_at(n)
        source = cot_t if piece == OUT else unit_t

        right = attended[...] if piece == OUT else back[piece]
        size = plane // CORES
        for at in range(CORES):
            rows = pl.ds(pl.multiple_of(target * plane + at * size, size), size)
            terms[piece, rows, :] = dot(source[rows, :], right).astype(BF16)

        for step in range(1, chip_count):
            t_beside(piece, target, (chip + step) % chip_count).start()
        t_beside(piece, target, chip).start()

    def send_across(piece, n):
        target = target_at(n)
        for step in range(1, chip_count):
            other = (chip + step) % chip_count
            t_beside(piece, target, other).wait_recv()
            own = target * dp_count + other * CORES + core
            add_into(held, piece, target * chip_count + other, [(terms, own)], own_rows)
            t_across(piece, target, step).start()

    def terms_out(piece):
        for n in range(seq_count):
            make_terms(piece, n)
            if n > 0:
                send_across(piece, n - 1)
        send_across(piece, seq_count - 1)

    def gather_y(piece, n):
        target = target_at(n)
        t_beside(piece, target, chip).wait_recv()
        others = [(terms, target * dp_count + index)]
        for step in range(1, chip_count):
            t_across(piece, target, step).wait_recv()
            others.append((chip_in, (step - 1) * seq_count + target))
        add_into(held, piece, target * chip_count + chip, others, own_rows)

        @pl.when((target > place) & (place == 0))
        def _():
            t_chain(piece, target, True).start()

        @pl.when((target < place) & (place == seq_count - 1))
        def _():
            t_chain(piece, target, False).start()

    def pass_z(piece, n):
        target = target_at(n)
        slot = target * chip_count + chip

        @pl.when((place < target) & not_first)
        def _():
            t_chain(piece, target, True).wait_recv()
            add_into(held, piece, slot, [(chain_in, target)], own_rows)
            t_chain(piece, target, True).start()

        @pl.when((place > target) & not_last)
        def _():
            t_chain(piece, target, False).wait_recv()
            add_into(held, piece, slot, [(chain_in, target)], own_rows)
            t_chain(piece, target, False).start()

    width = next(size for size in (512, 384, 256, 128) if share % size == 0)

    def lanes(values):
        total = values[:, :128]
        for at in range(128, width, 128):
            total = total + values[:, at : at + 128]
        return total

    def x_copy(step):
        other = (lane + step) % tensor_count
        sems = x_send.at[step - 1], x_recv.at[step - 1]
        return remote(inner.at[other], inner_in.at[step - 1], *sems, {"tensor": other})

    def xs_copy(step):
        other = (lane + step) % tensor_count
        sems = xs_send.at[step - 1], xs_recv.at[step - 1]
        return remote(sum_rows, sum_rows_in.at[step - 1], *sems, {"tensor": other})

    def inner_grad():
        sums[...] = jnp.zeros_like(sums)

        def tile(owner, step):
            start = owner * share + step * width
            cut = pl.ds(pl.multiple_of(start, width), width)
            product = dot_nt(back[QUERY], weights[QUERY, cut, :])
            product = product + dot_nt(back[KEY], weights[KEY, cut, :])
            product = product + dot_nt(back[VALUE], weights[VALUE, cut, :])
            unit = (tok[:, cut].astype(F32) - stat_mean[:, :1]) * stat_inv[:, :1]
            sums[0] += lanes(product)
            sums[1] += lanes(product * unit)
            at = pl.ds(pl.multiple_of(step * width, width), width)
            inner[owner, :, at] = product.astype(BF16)

        for turn in range(1, tensor_count + 1):

            @pl.loop(0, share // width)
            def _(step):
                tile((lane + turn) % tensor_count, step)

            if turn < tensor_count:
                x_copy(turn).start()
        sum_rows[...] = jnp.zeros_like(sum_rows)
        for at in range(2):
            sum_rows[at : at + 1, :] = jnp.sum(sums[at].T, axis=0, keepdims=True)
        for step in range(1, tensor_count):
            xs_copy(step).start()

    def finish_branch():
        for step in range(1, tensor_count):
            x_copy(step).wait_recv()
            xs_copy(step).wait_recv()
        total = sum_rows[...]
        for other in range(tensor_count - 1):
            total = total + sum_rows_in[other]
        sum_columns[...] = total.T / feature_count

        @pl.loop(0, token_count // 16)
        def _(step):
            rows = pl.ds(pl.multiple_of(step * 16, 16), 16)
            values = inner[lane, rows, :].astype(F32)
            for other in range(tensor_count - 1):
                values = values + inner_in[other, rows, :].astype(F32)
            means = sum_columns[rows, :]
            mean_grad, mean_both = means[:, 0:1], means[:, 1:2]
            cut = pl.ds(pl.multiple_of(lane * share, share), share)
            inverse = stat_inv[rows, :][:, :1]
            unit = (tok[rows, cut].astype(F32) - stat_mean[rows, :][:, :1]) * inverse
            branch_out[rows, :] = ((values - mean_grad - unit * mean_both) * inverse).astype(BF16)

    def finish_weights(piece):
        own_held = place * chip_count + chip

        @pl.when(not_first)
        def _():
            t_chain(piece, place, True).wait_recv()

        @pl.when(not_last)
        def _():
            t_chain(piece, place, False).wait_recv()

        @pl.loop(0, own_rows // 16)
        def _(step):
            rows = pl.ds(pl.multiple_of(step * 16, 16), 16)

            def cut(at):
                return pl.ds(pl.multiple_of(at * own_rows + step * 16, 16), 16)

            summed[piece, rows, :] = held[piece, cut(own_held), :].astype(F32)

            @pl.when(not_first)
            def _():
                summed[piece, rows, :] += chain_in[piece, cut(place), :].astype(F32)

            @pl.when(not_last)
            def _():
                summed[piece, rows, :] += chain_in[piece, cut(seq_count), :].astype(F32)

    def out_copy(piece):
        target = outw_out if piece == OUT else qkv_out.at[(1, 2, 0)[piece]]
        return pltpu.make_async_copy(summed.at[piece], target, store_sem.at[piece])

    def branch_copy():
        return pltpu.make_async_copy(branch_out, branch_hbm, store_sem.at[4])

    for n in range(seq_count):
        backward(n)
        g_first(0, n)
        if n == min(1, seq_count - 1):
            terms_out(OUT)
    for n in range(seq_count):
        g_first(1, n)
    back_query()
    terms_out(QUERY)
    for n in range(seq_count):
        gather_y(OUT, n)
    for n in range(seq_count - 1):
        g_step(0, n)
    g_own(0)
    back_keys()
    terms_out(KEY)
    for n in range(seq_count - 1):
        g_step(1, n)
    g_own(1)
    back_values()
    terms_out(VALUE)
    for n in range(seq_count):
        gather_y(QUERY, n)
    pass_z(OUT, 0)
    inner_grad()
    for n in range(1, seq_count - 1):
        pass_z(OUT, n)
    for n in range(seq_count):
        gather_y(KEY, n)
        if n < seq_count - 1:
            pass_z(QUERY, n)
    for n in range(seq_count):
        gather_y(VALUE, n)
        if n < seq_count - 1:
            pass_z(KEY, n)
    for n in range(seq_count - 1):
        pass_z(VALUE, n)
    for piece in (OUT, QUERY, KEY):
        finish_weights(piece)
        out_copy(piece).start()
    finish_branch()
    branch_copy().start()
    finish_weights(VALUE)
    out_copy(VALUE).start()
    for piece in range(4):
        out_copy(piece).wait()
    branch_copy().wait()

    def drain():
        for origin in range(seq_count):
            to_right = (origin <= place) & not_last
            to_left = (origin >= place) & not_first
            for piece in range(4):
                for step in range(1, chip_count):
                    w_across(piece, origin, step).wait_send()
                    t_across(piece, origin, step).wait_send()
                for source_chip in range(chip_count):
                    w_beside(piece, origin, source_chip).wait_send()
                    t_beside(piece, origin, source_chip).wait_send()

                @pl.when(to_right)
                def _():
                    w_side(piece, origin, True).wait_send()

                @pl.when(to_left)
                def _():
                    w_side(piece, origin, False).wait_send()

                @pl.when(place != origin)
                def _():
                    t_chain(piece, origin, True).wait_send()

            for piece in range(2):

                @pl.when(to_right)
                def _():
                    p_copy(piece, origin, True).wait_send()

                @pl.when(to_left)
                def _():
                    p_copy(piece, origin, False).wait_send()

                @pl.when(place != origin)
                def _():
                    g_copy(piece, origin, True).wait_send()

        for step in range(1, tensor_count):
            x_copy(step).wait_send()
            xs_copy(step).wait_send()

    drain()


def local(tokens, cotangent, qkv_weight, out_weight):
    seq_count, dp_count = lax.axis_size("seq"), lax.axis_size("dp")
    tensor_count = lax.axis_size("tensor")
    chip_count = dp_count // CORES
    row_count, feature_count = tokens.shape[1:]
    own_rows, columns = out_weight.shape
    head_count = columns // HD
    share = feature_count // tensor_count
    sizes = (seq_count, dp_count, tensor_count, own_rows, head_count)

    def vmem(*shape, kind=BF16):
        return pltpu.VMEM(shape, kind)

    def dma(*shape):
        return pltpu.SemaphoreType.DMA(shape)

    both, peers = seq_count * chip_count, seq_count * max(chip_count - 1, 1)
    others = max(tensor_count - 1, 1)
    scratch = [
        vmem(row_count, feature_count),
        vmem(row_count, feature_count),
        vmem(row_count, feature_count),
        vmem(feature_count, row_count),
        vmem(feature_count, row_count),
        vmem(row_count, 128, kind=F32),
        vmem(row_count, 128, kind=F32),
        vmem(4, feature_count, columns),
        vmem(4, row_count, columns, kind=F32),
        vmem(2, seq_count * row_count, columns),
        vmem(row_count, columns),
        vmem(row_count, columns, kind=F32),
        vmem(row_count, columns, kind=F32),
        vmem(row_count, columns, kind=F32),
        vmem(row_count, columns, kind=F32),
        vmem(row_count, columns),
        vmem(head_count * seq_count * row_count, row_count),
        vmem(head_count, row_count, HD, kind=F32),
        vmem(head_count, row_count, HD, kind=F32),
        vmem(row_count, columns, kind=F32),
        vmem(row_count, columns),
        vmem(row_count, columns, kind=F32),
        vmem(2, seq_count * row_count, columns),
        vmem(2, (seq_count + 1) * row_count, columns),
        vmem(3, row_count, columns),
        vmem(tensor_count, row_count, share),
        vmem(others, row_count, share),
        vmem(2, row_count, 128, kind=F32),
        vmem(4, feature_count, columns),
        vmem(4, both * own_rows, columns),
        vmem(4, peers * own_rows, columns),
        vmem(4, (seq_count + 1) * own_rows, columns),
        vmem(4, own_rows, columns, kind=F32),
        vmem(row_count, share),
        vmem(8, row_count, kind=F32),
        vmem(others, 8, row_count, kind=F32),
        vmem(row_count, 8, kind=F32),
        dma(5),
        dma(5),
        dma(4, seq_count * dp_count),
        dma(4, seq_count),
        dma(4, seq_count),
        dma(4, both),
        dma(4, both),
        dma(2, seq_count),
        dma(2, seq_count),
        dma(2, seq_count),
        dma(2, seq_count),
        dma(2, seq_count),
        dma(2, seq_count),
        dma(4, both),
        dma(4, both),
        dma(4, peers),
        dma(4, peers),
        dma(4, seq_count),
        dma(4, seq_count),
        dma(4, seq_count),
        dma(others),
        dma(others),
        dma(others),
        dma(others),
    ]
    anywhere = pl.BlockSpec(memory_space=pl.ANY)
    qkv_grad, out_grad, branch = pl.pallas_call(
        functools.partial(body, sizes),
        out_shape=(
            jax.ShapeDtypeStruct((3, own_rows, columns), F32),
            jax.ShapeDtypeStruct((own_rows, columns), F32),
            jax.ShapeDtypeStruct((row_count, share), BF16),
        ),
        in_specs=[anywhere] * 4,
        out_specs=(anywhere, anywhere, anywhere),
        scratch_shapes=scratch,
        compiler_params=pltpu.CompilerParams(
            collective_id=0, has_side_effects=True, vmem_limit_bytes=67043328
        ),
        name="layer",
    )(tokens[0], cotangent[0], jnp.transpose(qkv_weight, (1, 0, 2)), out_weight)
    return jnp.transpose(qkv_grad, (1, 0, 2)), out_grad, branch[None]


def solution(mesh):
    return jax.shard_map(
        local,
        mesh=mesh,
        in_specs=(
            P("dp", "seq", None),
            P("dp", "seq", None),
            P(("seq", "dp"), None, "tensor"),
            P(("seq", "dp"), "tensor"),
        ),
        out_specs=(
            P(("seq", "dp"), None, "tensor"),
            P(("seq", "dp"), "tensor"),
            P("dp", "seq", "tensor"),
        ),
        check_vma=False,
    )
```

```python
import functools

import jax
import jax.numpy as jnp
from jax import lax
from jax.experimental import pallas as pl
from jax.experimental.pallas import tpu as pltpu
from jax.sharding import PartitionSpec as P

HD = 128
CORES = 2
MESH_ID = pl.DeviceIdType.MESH
EPSILON = 1e-06
F32, BF16 = jnp.float32, jnp.bfloat16


(
    W_KV,
    OWN_QUERY,
    SPREAD_QUERY,
    CHIP_KV,
    MIX_KV,
    KEY_READY,
    W_QO,
    SEND_PAIRS,
    FLIP_UNIT,
    FLIP_COT,
    CHIP_QO,
    MIX_QO,
    PAIR,
    QUERY_READY,
    ATTEND,
    ATTEND_END,
    BACKWARD,
    FIRST_KEY,
    FIRST_VALUE,
    MAKE_OUT,
    ACROSS_OUT,
    BACK_QUERY,
    MAKE_QUERY,
    ACROSS_QUERY,
    Y_OUT,
    G_KEY,
    OWN_KEY,
    BACK_KEYS,
    MAKE_KEY,
    ACROSS_KEY,
    G_VALUE,
    OWN_VALUE,
    BACK_VALUES,
    MAKE_VALUE,
    ACROSS_VALUE,
    Y_QUERY,
    Z_OUT,
    INNER_GRAD,
    Y_KEY,
    Z_QUERY,
    Y_VALUE,
    Z_KEY,
    Z_VALUE,
    FINISH_OUT,
    FINISH_QUERY,
    FINISH_KEY,
    FINISH_BRANCH,
    FINISH_VALUE,
) = range(48)
FORWARD_TIMES = {
    W_KV: (-4.87, 5.57),
    OWN_QUERY: (-12.55, 3.56),
    SPREAD_QUERY: (27.94, 1.11),
    CHIP_KV: (11.34, 3.56),
    MIX_KV: (29.29, 1.26),
    KEY_READY: (20.32, 0.0),
    W_QO: (26.16, 3.27),
    SEND_PAIRS: (26.3, 0.47),
    FLIP_UNIT: (52.59, 0.0),
    FLIP_COT: (19.92, 1.65),
    CHIP_QO: (37.05, 3.63),
    MIX_QO: (34.13, 6.34),
    PAIR: (42.23, 6.16),
    QUERY_READY: (67.43, 6.51),
    ATTEND: (45.34, 0.0),
    ATTEND_END: (77.44, 0.0),
}
BACKWARD_TIMES = {
    BACKWARD: (-2.19, 2.64),
    FIRST_KEY: (-2.46, 1.91),
    FIRST_VALUE: (6.2, 0.54),
    MAKE_OUT: (1.52, 0.0),
    ACROSS_OUT: (4.71, 0.17),
    BACK_QUERY: (2.54, 0.0),
    MAKE_QUERY: (-18.11, 0.64),
    ACROSS_QUERY: (15.9, 0.82),
    Y_OUT: (18.34, 0.0),
    G_KEY: (3.85, 0.0),
    OWN_KEY: (18.05, 1.39),
    BACK_KEYS: (29.33, 0.5),
    MAKE_KEY: (2.07, 0.03),
    ACROSS_KEY: (9.4, 2.81),
    G_VALUE: (21.95, 2.42),
    OWN_VALUE: (32.26, 0.0),
    BACK_VALUES: (47.91, 1.68),
    MAKE_VALUE: (15.23, 0.0),
    ACROSS_VALUE: (45.49, 1.78),
    Y_QUERY: (38.62, 4.26),
    Z_OUT: (30.05, 5.94),
    INNER_GRAD: (52.42, 4.91),
    Y_KEY: (46.6, 6.84),
    Z_QUERY: (51.97, 0.56),
    Y_VALUE: (59.28, 0.83),
    Z_KEY: (53.48, 2.55),
    Z_VALUE: (65.73, 6.14),
    FINISH_OUT: (83.86, 0.52),
    FINISH_QUERY: (68.47, 0.33),
    FINISH_KEY: (78.69, 2.43),
    FINISH_BRANCH: (89.16, 1.92),
    FINISH_VALUE: (92.27, 0.0),
}


PIECES = (
    (BACK_KEYS, MAKE_KEY, ACROSS_KEY, Y_KEY, Z_KEY, FINISH_KEY),
    (BACK_VALUES, MAKE_VALUE, ACROSS_VALUE, Y_VALUE, Z_VALUE, FINISH_VALUE),
    (BACK_QUERY, MAKE_QUERY, ACROSS_QUERY, Y_QUERY, Z_QUERY, FINISH_QUERY),
    (None, MAKE_OUT, ACROSS_OUT, Y_OUT, Z_OUT, FINISH_OUT),
)


def events_until(k, seq_count):
    return min(2 * (seq_count - 1), 4 * ((k + 1) // 2))


def forward_steps(seq_count):
    events = 2 * (seq_count - 1)
    needs = {(OWN_QUERY, 0): [(W_KV, min(4, events) - 1)] if events else [], (SPREAD_QUERY, 0): []}
    for come, across, mix in ((W_KV, CHIP_KV, MIX_KV), (W_QO, CHIP_QO, MIX_QO)):
        for n in range(events):
            needs[come, n] = [(come, n - 1)] if n else []
        for n in range(events + 2):
            needs[across, n] = [(across, n - 1)] if n else []
            if n > 1:
                needs[across, n].append((come, n - 2))
        for k in range(seq_count):
            needs[mix, k] = [(across, 1 + events_until(k, seq_count))]
            if k:
                needs[mix, k].append((mix, k - 1))
    for n in range(2):
        needs[CHIP_QO, n].append((SPREAD_QUERY, 0))
    if events:
        needs[W_QO, 0] = [(OWN_QUERY, 1)]
    needs[OWN_QUERY, 1] = [(OWN_QUERY, 0)] + ([(W_KV, events - 1)] if events else [])
    needs[KEY_READY, 0] = [(MIX_KV, seq_count - 1)]
    needs[SEND_PAIRS, 0] = [(KEY_READY, 0)]
    needs[FLIP_UNIT, 0] = needs[FLIP_COT, 0] = []
    for n in range(events):
        needs[PAIR, n] = [(PAIR, n - 1) if n else (SEND_PAIRS, 0)]
    needs[QUERY_READY, 0] = [(MIX_QO, seq_count - 1)]
    for k in range(seq_count):
        needs[ATTEND, k] = [(ATTEND, k - 1) if k else (QUERY_READY, 0), (KEY_READY, 0)]
        if events_until(k, seq_count):
            needs[ATTEND, k].append((PAIR, events_until(k, seq_count) - 1))
    ends = [(ATTEND, seq_count - 1), (FLIP_UNIT, 0), (FLIP_COT, 0)]
    needs[ATTEND_END, 0] = ends
    return in_order(needs, FORWARD_TIMES)


def backward_steps(seq_count):
    needs, last = {}, seq_count - 1

    def chained(name, count, more):
        for n in range(count):
            needs[name, n] = ([(name, n - 1)] if n else []) + more(n)

    chained(BACKWARD, seq_count, lambda n: [])
    for first, come, own in ((FIRST_KEY, G_KEY, OWN_KEY), (FIRST_VALUE, G_VALUE, OWN_VALUE)):
        chained(first, seq_count, lambda n: [(BACKWARD, n)])
        chained(come, last, lambda n: [(first, last)])
        needs[own, 0] = [(come, last - 1) if last else (first, last)]
    needs[BACK_QUERY, 0] = [(BACKWARD, last)]
    needs[BACK_KEYS, 0] = [(OWN_KEY, 0)]
    needs[BACK_VALUES, 0] = [(OWN_VALUE, 0)]
    for ready, make, across, come, chain, finish in PIECES:
        first = [] if ready is None else [(ready, 0)]
        chained(make, seq_count, lambda n: first)
        chained(across, seq_count, lambda n: [(make, n)])
        chained(come, seq_count, lambda n: [(across, n)])
        chained(chain, last, lambda n: [(come, n)])
        needs[finish, 0] = [(come, last)] + ([(chain, last - 1)] if last else [])
    needs[INNER_GRAD, 0] = [(BACK_VALUES, 0), (BACK_KEYS, 0), (BACK_QUERY, 0)]
    needs[FINISH_BRANCH, 0] = [(INNER_GRAD, 0)]
    return in_order(needs, BACKWARD_TIMES)


def in_order(needs, times):
    left, steps = dict(needs), []
    while left:
        able = [step for step in left if not any(other in left for other in left[step])]
        best = min(able, key=lambda step: (times[step[0]][0] + times[step[0]][1] * step[1], step))
        steps.append(best)
        del left[best]
    return steps


def dot(left, right):
    return jnp.dot(left, right, preferred_element_type=F32)


def dot_nt(left, right):
    return lax.dot_general(left, right, (((1,), (1,)), ((), ())), preferred_element_type=F32)


def dot_tn(left, right):
    return lax.dot_general(left, right, (((0,), (0,)), ((), ())), preferred_element_type=F32)


def normalize(values):
    centered = values - jnp.mean(values, axis=-1, keepdims=True)
    inverse = lax.rsqrt(jnp.mean(centered * centered, axis=-1, keepdims=True) + EPSILON)
    return centered * inverse, inverse


def normalize_back(gradient, normed, inverse):
    mean_grad = jnp.mean(gradient, axis=-1, keepdims=True)
    mean_both = jnp.mean(gradient * normed, axis=-1, keepdims=True)
    return (gradient - mean_grad - normed * mean_both) * inverse


def body(
    sizes,
    tokens_hbm,
    cotangent_hbm,
    qkv_hbm,
    outw_hbm,
    qkv_out,
    outw_out,
    branch_hbm,
    tok,
    cot,
    unit_low,
    unit_t,
    cot_t,
    stat_mean,
    stat_inv,
    weights,
    acc,
    pairs,
    query_low,
    query_unit,
    key_unit,
    query_inv,
    key_inv,
    grad_low,
    expo,
    totals,
    deltas,
    weighted,
    attended,
    query_raw,
    part,
    part_in,
    back,
    inner,
    inner_in,
    sums,
    terms,
    held,
    chip_in,
    chain_in,
    summed,
    branch_out,
    sum_rows,
    sum_rows_in,
    sum_columns,
    load_sem,
    store_sem,
    w_recv,
    w_send,
    p_recv,
    p_send,
    g_low,
    g_high,
    g_send,
    t_core_recv,
    t_chip_recv,
    t_send,
    t_low_recv,
    t_high_recv,
    x_send,
    x_recv,
    xs_send,
    xs_recv,
):
    seq_count, dp_count, tensor_count, own_rows, head_count = sizes
    chip_count = dp_count // CORES
    token_count, feature_count = tok.shape
    share = feature_count // tensor_count
    plane = dp_count * own_rows
    scale = HD ** (-0.5)
    place = lax.axis_index("seq")
    index = lax.axis_index("dp")
    lane = lax.axis_index("tensor")
    chip, core = index // CORES, index % CORES
    not_last, not_first = place < seq_count - 1, place > 0
    both_sides = jnp.minimum(place, seq_count - 1 - place)
    KEY, VALUE, QUERY, OUT = range(4)

    def rows_of(slot):
        return pl.ds(pl.multiple_of(slot * own_rows, own_rows), own_rows)

    def block_rows(origin):
        return pl.ds(pl.multiple_of(origin * token_count, token_count), token_count)

    own_rows_at = rows_of(place * dp_count + index)
    loads = [
        pltpu.make_async_copy(
            qkv_hbm.at[pl.ds(1, 2)], weights.at[pl.ds(0, 2), own_rows_at, :], load_sem.at[0]
        ),
        pltpu.make_async_copy(qkv_hbm.at[0], weights.at[QUERY, own_rows_at, :], load_sem.at[1]),
        pltpu.make_async_copy(outw_hbm, weights.at[OUT, own_rows_at, :], load_sem.at[2]),
        pltpu.make_async_copy(tokens_hbm, tok, load_sem.at[3]),
        pltpu.make_async_copy(cotangent_hbm, cot, load_sem.at[4]),
    ]
    for load in loads:
        load.start()

    barrier = pltpu.get_barrier_semaphore()

    def signal(device):
        pl.semaphore_signal(barrier, inc=1, device_id=device, device_id_type=MESH_ID)

    def greet():
        @pl.when(not_first)
        def _():
            signal({"seq": place - 1})

        @pl.when(not_last)
        def _():
            signal({"seq": place + 1})

        for step in range(1, chip_count):
            signal({"dp": (chip + step) % chip_count * CORES + core})
        signal({"dp": chip * CORES + 1 - core})
        for step in range(1, tensor_count):
            signal({"tensor": (lane + step) % tensor_count})
        ends = jnp.minimum(place, 1) + jnp.minimum(seq_count - 1 - place, 1)
        pl.semaphore_wait(barrier, chip_count + tensor_count - 1 + ends)

    greet()

    def remote(source, target, send_sem, recv_sem, device):
        return pltpu.make_async_remote_copy(
            src_ref=source,
            dst_ref=target,
            send_sem=send_sem,
            recv_sem=recv_sem,
            device_id=device,
            device_id_type=MESH_ID,
        )

    up, down = {"seq": place + 1}, {"seq": place - 1}
    beside_device = {"dp": chip * CORES + 1 - core}

    def chip_device(step):
        return {"dp": (chip + step) % chip_count * CORES + core}

    def origin_at(k):
        near = jnp.where(k % 2 == 1, place - (k + 1) // 2, place + k // 2)
        far = jnp.where(
            place * 2 > seq_count - 1, place - (k - both_sides), place + (k - both_sides)
        )
        return jnp.where(k <= 2 * both_sides, near, far)

    def event(number):
        group, rest = number // 4, number % 4
        if 2 * group + 2 <= seq_count - 1:
            paired = both_sides > group
            piece = jnp.where(paired, rest // 2, rest % 2)
            k = 2 * group + 1 + jnp.where(paired, rest % 2, rest // 2)
        else:
            piece, k = rest % 2, 2 * group + 1 + rest // 2
        return piece, origin_at(k)

    def w_copy(piece, slot, send_sem, device):
        ref = weights.at[piece, rows_of(slot), :]
        return remote(ref, ref, send_sem, w_recv.at[piece, slot], device)

    def w_side(piece, origin, rightward):
        if rightward:
            return w_copy(piece, origin * dp_count + index, w_send.at[0], up)
        return w_copy(piece, origin * dp_count + index, w_send.at[0], down)

    def w_across(piece, origin, step):
        return w_copy(piece, origin * dp_count + index, w_send.at[1], chip_device(step))

    def w_beside(piece, origin, source_chip):
        slot = origin * dp_count + source_chip * CORES + core
        return w_copy(piece, slot, w_send.at[2], beside_device)

    def w_landed(piece, slot):
        w_copy(piece, slot, w_send.at[2], beside_device).wait_recv()

    def w_sides_own(first):
        for piece in (first, first + 1):

            @pl.when(not_last)
            def _():
                w_side(piece, place, True).start()

            @pl.when(not_first)
            def _():
                w_side(piece, place, False).start()

    def w_spread_own(first):
        for piece in (first, first + 1):
            for step in range(1, chip_count):
                w_across(piece, place, step).start()
        for piece in (first, first + 1):
            w_beside(piece, place, chip).start()

    def w_step(first, number):
        piece, origin = event(number)
        piece = piece + first
        w_landed(piece, origin * dp_count + index)

        @pl.when((origin < place) & not_last)
        def _():
            w_side(piece, origin, True).start()

        @pl.when((origin > place) & not_first)
        def _():
            w_side(piece, origin, False).start()

        for step in range(1, chip_count):
            w_across(piece, origin, step).start()
        w_beside(piece, origin, chip).start()

    def w_chip_step(first, number):
        piece, origin = (number, place) if number < 2 else event(number - 2)
        piece = piece + first
        for step in range(1, chip_count):
            source_chip = (chip + step) % chip_count
            w_landed(piece, origin * dp_count + source_chip * CORES + core)
            w_beside(piece, origin, source_chip).start()

    def project(first, k):
        origin = origin_at(k)
        rows = pl.ds(pl.multiple_of(origin * plane, plane), plane)
        for piece in (first, first + 1):
            for source_chip in range(chip_count):
                w_landed(piece, origin * dp_count + source_chip * CORES + 1 - core)
        for piece in (first, first + 1):
            source = cot if piece == OUT else unit_low
            product = dot(source[:, rows], weights[piece, rows, :])
            if k == 0:
                acc[piece] = product
            else:
                acc[piece] += product

    def p_copy(piece, origin, rightward):
        ref = pairs.at[piece, block_rows(origin), :]
        if rightward:
            return remote(ref, ref, p_send.at[0], p_recv.at[piece, origin], up)
        return remote(ref, ref, p_send.at[0], p_recv.at[piece, origin], down)

    def p_step(number):
        piece, origin = event(number)
        p_copy(piece, origin, True).wait_recv()

        @pl.when((origin < place) & not_last)
        def _():
            p_copy(piece, origin, True).start()

        @pl.when((origin > place) & not_first)
        def _():
            p_copy(piece, origin, False).start()

    def p_sides_own():
        for piece in range(2):

            @pl.when(not_last)
            def _():
                p_copy(piece, place, True).start()

            @pl.when(not_first)
            def _():
                p_copy(piece, place, False).start()

    def normalize_tokens():
        @pl.loop(0, token_count // 32)
        def _(step):
            rows = pl.ds(pl.multiple_of(step * 32, 32), 32)
            values = tok[rows, :].astype(F32)
            average = jnp.mean(values, axis=-1, keepdims=True)
            centered = values - average
            inverse = lax.rsqrt(jnp.mean(centered * centered, axis=-1, keepdims=True) + EPSILON)
            unit_low[rows, :] = (centered * inverse).astype(BF16)
            stat_mean[rows, :] = jnp.broadcast_to(average, (32, 128))
            stat_inv[rows, :] = jnp.broadcast_to(inverse, (32, 128))

    def flip(source, target):
        @pl.loop(0, feature_count // 128)
        def _(step):
            cut = pl.ds(pl.multiple_of(step * 128, 128), 128)
            target[cut, :] = source[:, cut].T

    def key_ready():
        own_block = block_rows(place)
        for h in range(head_count):
            cut = slice(h * HD, (h + 1) * HD)
            normed, inverse = normalize(acc[KEY, :, cut])
            key_unit[:, cut] = normed
            key_inv[:, cut] = jnp.broadcast_to(inverse, (token_count, HD))
            pairs[0, own_block, cut] = normed.astype(BF16)
            pairs[1, own_block, cut] = acc[VALUE, :, cut].astype(BF16)

    def query_ready():
        for h in range(head_count):
            cut = slice(h * HD, (h + 1) * HD)
            normed, inverse = normalize(acc[QUERY, :, cut])
            query_unit[:, cut] = normed
            query_inv[:, cut] = jnp.broadcast_to(inverse, (token_count, HD))
            query_low[:, cut] = normed.astype(BF16)
        grad_low[...] = acc[OUT].astype(BF16)

    loads[0].wait()
    w_sides_own(KEY)
    w_spread_own(KEY)
    for load in loads[1:]:
        load.wait()
    normalize_tokens()

    def head_cut(h):
        return pl.ds(pl.multiple_of(h * HD, HD), HD)

    def expo_at(origin, h):
        row = (h * seq_count + origin) * token_count
        return pl.ds(pl.multiple_of(row, token_count), token_count)

    def attend(k):
        origin = origin_at(k)

        @pl.loop(0, head_count)
        def _(h):
            cut = head_cut(h)
            rows = block_rows(origin)
            scores = dot_nt(query_low[:, cut], pairs[0, rows, cut]) * scale
            exponent = jnp.exp(scores)
            low = exponent.astype(BF16)
            expo[expo_at(origin, h), :] = low
            total = exponent[:, :HD]
            for at in range(HD, token_count, HD):
                total = total + exponent[:, at : at + HD]
            mixed = dot(low, pairs[1, rows, cut])
            if k == 0:
                totals[h] = total
                weighted[:, cut] = mixed
            else:
                totals[h] += total
                weighted[:, cut] += mixed

    def attend_end():
        for h in range(head_count):
            cut = slice(h * HD, (h + 1) * HD)
            total = jnp.sum(totals[h], axis=-1, keepdims=True)
            low = (weighted[:, cut] / total).astype(BF16)
            attended[:, cut] = low
            both = grad_low[:, cut].astype(F32) * low.astype(F32)
            totals[h] = jnp.broadcast_to(1.0 / total, (token_count, HD))
            deltas[h] = jnp.broadcast_to(jnp.sum(both, axis=-1, keepdims=True), (token_count, HD))

    at_end = both_sides == 0

    def own_query(number):
        @pl.when(jnp.logical_not(at_end) if number else at_end)
        def _():
            w_sides_own(QUERY)

    ahead = {
        W_KV: lambda n: w_step(KEY, n),
        OWN_QUERY: own_query,
        SPREAD_QUERY: lambda n: w_spread_own(QUERY),
        CHIP_KV: lambda n: w_chip_step(KEY, n),
        MIX_KV: lambda n: project(KEY, n),
        KEY_READY: lambda n: key_ready(),
        W_QO: lambda n: w_step(QUERY, n),
        SEND_PAIRS: lambda n: p_sides_own(),
        FLIP_UNIT: lambda n: flip(unit_low, unit_t),
        FLIP_COT: lambda n: flip(cot, cot_t),
        CHIP_QO: lambda n: w_chip_step(QUERY, n),
        MIX_QO: lambda n: project(QUERY, n),
        PAIR: p_step,
        QUERY_READY: lambda n: query_ready(),
        ATTEND: attend,
        ATTEND_END: lambda n: attend_end(),
    }
    for name, number in forward_steps(seq_count):
        ahead[name](number)

    def target_at(n):
        return origin_at(seq_count - 1 - n)

    def from_above(target, receiver):
        return jnp.where(target == receiver, seq_count, target)

    def add_into(ref, piece, slot, others, size):
        @pl.loop(0, size // 16)
        def _(step):
            def cut(at):
                return pl.ds(pl.multiple_of(at * size + step * 16, 16), 16)

            total = ref[piece, cut(slot), :].astype(F32)
            for other, at in others:
                total = total + other[piece, cut(at), :].astype(F32)
            ref[piece, cut(slot), :] = total.astype(BF16)

    def g_copy(piece, target, rightward):
        rows = block_rows(target)
        source = part.at[piece, rows, :]
        if rightward:
            into, sem, device = rows, g_low, up
        else:
            into, sem, device = block_rows(from_above(target, place - 1)), g_high, down
        into = part_in.at[piece, into, :]
        return remote(source, into, g_send.at[0], sem.at[piece, target], device)

    def backward(n):
        target = target_at(n)

        @pl.loop(0, head_count)
        def _(h):
            cut = head_cut(h)
            rows = block_rows(target)
            inv_total = totals[h][:, :1]
            probability = expo[expo_at(target, h), :].astype(F32) * inv_total
            gradient = grad_low[:, cut]
            prob_grad = dot_nt(gradient, pairs[1, rows, cut])
            score = (probability * (prob_grad - deltas[h][:, :1]) * scale).astype(BF16)
            query_part = dot(score, pairs[0, rows, cut])
            part[0, rows, cut] = dot_tn(score, query_low[:, cut]).astype(BF16)
            part[1, rows, cut] = dot_tn(probability.astype(BF16), gradient).astype(BF16)
            if n == 0:
                query_raw[:, cut] = query_part
            else:
                query_raw[:, cut] += query_part

    def g_first(piece, n):
        target = target_at(n)

        @pl.when((target > place) & (place == 0))
        def _():
            g_copy(piece, target, True).start()

        @pl.when((target < place) & (place == seq_count - 1))
        def _():
            g_copy(piece, target, False).start()

    def g_step(piece, n):
        target = target_at(n)

        @pl.when((place < target) & not_first)
        def _():
            g_copy(piece, target, True).wait_recv()
            add_into(part, piece, target, [(part_in, target)], token_count)
            g_copy(piece, target, True).start()

        @pl.when((place > target) & not_last)
        def _():
            g_copy(piece, target, False).wait_recv()
            add_into(part, piece, target, [(part_in, target)], token_count)
            g_copy(piece, target, False).start()

    def g_own(piece):
        @pl.when(not_first)
        def _():
            g_copy(piece, place, True).wait_recv()
            add_into(part, piece, place, [(part_in, place)], token_count)

        @pl.when(not_last)
        def _():
            g_copy(piece, place, False).wait_recv()
            add_into(part, piece, place, [(part_in, seq_count)], token_count)

    def back_query():
        for h in range(head_count):
            cut = slice(h * HD, (h + 1) * HD)
            raised = normalize_back(query_raw[:, cut], query_unit[:, cut], query_inv[:, cut])
            back[QUERY, :, cut] = raised.astype(BF16)

    def back_keys():
        own_block = block_rows(place)
        for h in range(head_count):
            cut = slice(h * HD, (h + 1) * HD)
            raw = part[0, own_block, cut].astype(F32)
            raised = normalize_back(raw, key_unit[:, cut], key_inv[:, cut])
            back[KEY, :, cut] = raised.astype(BF16)

    def back_values():
        back[VALUE] = part[1, block_rows(place), :]

    def t_beside(piece, target, target_chip):
        slot = target * chip_count + target_chip
        source = terms.at[piece, rows_of(target * dp_count + target_chip * CORES + 1 - core), :]
        into = held.at[piece, rows_of(slot), :]
        sems = t_send.at[0], t_core_recv.at[piece, slot]
        return remote(source, into, *sems, beside_device)

    def t_across(piece, target, step):
        other = (chip + step) % chip_count
        slot = (step - 1) * seq_count + target
        source = held.at[piece, rows_of(target * chip_count + other), :]
        into = chip_in.at[piece, rows_of(slot), :]
        sems = t_send.at[1], t_chip_recv.at[piece, slot]
        return remote(source, into, *sems, chip_device(step))

    def t_chain(piece, target, rightward):
        source = held.at[piece, rows_of(target * chip_count + chip), :]
        if rightward:
            at, sem, device = target, t_low_recv, up
        else:
            at, sem, device = from_above(target, place - 1), t_high_recv, down
        into = chain_in.at[piece, rows_of(at), :]
        return remote(source, into, t_send.at[2], sem.at[piece, target], device)

    def make_terms(piece, n):
        target = target_at(n)
        source = cot_t if piece == OUT else unit_t

        right = attended[...] if piece == OUT else back[piece]
        size = plane // CORES
        for at in range(CORES):
            rows = pl.ds(pl.multiple_of(target * plane + at * size, size), size)
            terms[piece, rows, :] = dot(source[rows, :], right).astype(BF16)

        for step in range(1, chip_count):
            t_beside(piece, target, (chip + step) % chip_count).start()
        t_beside(piece, target, chip).start()

    def send_across(piece, n):
        target = target_at(n)
        for step in range(1, chip_count):
            other = (chip + step) % chip_count
            t_beside(piece, target, other).wait_recv()
            own = target * dp_count + other * CORES + core
            add_into(held, piece, target * chip_count + other, [(terms, own)], own_rows)
            t_across(piece, target, step).start()

    def gather_y(piece, n):
        target = target_at(n)
        t_beside(piece, target, chip).wait_recv()
        others = [(terms, target * dp_count + index)]
        for step in range(1, chip_count):
            t_across(piece, target, step).wait_recv()
            others.append((chip_in, (step - 1) * seq_count + target))
        add_into(held, piece, target * chip_count + chip, others, own_rows)

        @pl.when((target > place) & (place == 0))
        def _():
            t_chain(piece, target, True).start()

        @pl.when((target < place) & (place == seq_count - 1))
        def _():
            t_chain(piece, target, False).start()

    def pass_z(piece, n):
        target = target_at(n)
        slot = target * chip_count + chip

        @pl.when((place < target) & not_first)
        def _():
            t_chain(piece, target, True).wait_recv()
            add_into(held, piece, slot, [(chain_in, target)], own_rows)
            t_chain(piece, target, True).start()

        @pl.when((place > target) & not_last)
        def _():
            t_chain(piece, target, False).wait_recv()
            add_into(held, piece, slot, [(chain_in, target)], own_rows)
            t_chain(piece, target, False).start()

    width = next(size for size in (512, 384, 256, 128) if share % size == 0)

    def lanes(values):
        total = values[:, :128]
        for at in range(128, width, 128):
            total = total + values[:, at : at + 128]
        return total

    def x_copy(step):
        other = (lane + step) % tensor_count
        sems = x_send.at[step - 1], x_recv.at[step - 1]
        return remote(inner.at[other], inner_in.at[step - 1], *sems, {"tensor": other})

    def xs_copy(step):
        other = (lane + step) % tensor_count
        sems = xs_send.at[step - 1], xs_recv.at[step - 1]
        return remote(sum_rows, sum_rows_in.at[step - 1], *sems, {"tensor": other})

    def inner_grad():
        sums[...] = jnp.zeros_like(sums)

        def tile(owner, step):
            start = owner * share + step * width
            cut = pl.ds(pl.multiple_of(start, width), width)
            product = dot_nt(back[QUERY], weights[QUERY, cut, :])
            product = product + dot_nt(back[KEY], weights[KEY, cut, :])
            product = product + dot_nt(back[VALUE], weights[VALUE, cut, :])
            unit = (tok[:, cut].astype(F32) - stat_mean[:, :1]) * stat_inv[:, :1]
            sums[0] += lanes(product)
            sums[1] += lanes(product * unit)
            at = pl.ds(pl.multiple_of(step * width, width), width)
            inner[owner, :, at] = product.astype(BF16)

        for turn in range(1, tensor_count + 1):

            @pl.loop(0, share // width)
            def _(step):
                tile((lane + turn) % tensor_count, step)

            if turn < tensor_count:
                x_copy(turn).start()
        sum_rows[...] = jnp.zeros_like(sum_rows)
        for at in range(2):
            sum_rows[at : at + 1, :] = jnp.sum(sums[at].T, axis=0, keepdims=True)
        for step in range(1, tensor_count):
            xs_copy(step).start()

    def finish_branch():
        for step in range(1, tensor_count):
            x_copy(step).wait_recv()
            xs_copy(step).wait_recv()
        total = sum_rows[...]
        for other in range(tensor_count - 1):
            total = total + sum_rows_in[other]
        sum_columns[...] = total.T / feature_count

        @pl.loop(0, token_count // 16)
        def _(step):
            rows = pl.ds(pl.multiple_of(step * 16, 16), 16)
            values = inner[lane, rows, :].astype(F32)
            for other in range(tensor_count - 1):
                values = values + inner_in[other, rows, :].astype(F32)
            means = sum_columns[rows, :]
            mean_grad, mean_both = means[:, 0:1], means[:, 1:2]
            cut = pl.ds(pl.multiple_of(lane * share, share), share)
            inverse = stat_inv[rows, :][:, :1]
            unit = (tok[rows, cut].astype(F32) - stat_mean[rows, :][:, :1]) * inverse
            branch_out[rows, :] = ((values - mean_grad - unit * mean_both) * inverse).astype(BF16)

    def finish_weights(piece):
        own_held = place * chip_count + chip

        @pl.when(not_first)
        def _():
            t_chain(piece, place, True).wait_recv()

        @pl.when(not_last)
        def _():
            t_chain(piece, place, False).wait_recv()

        @pl.loop(0, own_rows // 16)
        def _(step):
            rows = pl.ds(pl.multiple_of(step * 16, 16), 16)

            def cut(at):
                return pl.ds(pl.multiple_of(at * own_rows + step * 16, 16), 16)

            summed[piece, rows, :] = held[piece, cut(own_held), :].astype(F32)

            @pl.when(not_first)
            def _():
                summed[piece, rows, :] += chain_in[piece, cut(place), :].astype(F32)

            @pl.when(not_last)
            def _():
                summed[piece, rows, :] += chain_in[piece, cut(seq_count), :].astype(F32)

    def out_copy(piece):
        target = outw_out if piece == OUT else qkv_out.at[(1, 2, 0)[piece]]
        return pltpu.make_async_copy(summed.at[piece], target, store_sem.at[piece])

    def branch_copy():
        return pltpu.make_async_copy(branch_out, branch_hbm, store_sem.at[4])

    def finish(piece):
        finish_weights(piece)
        out_copy(piece).start()

    def branch_end():
        finish_branch()
        branch_copy().start()

    behind = {
        BACKWARD: backward,
        FIRST_KEY: lambda n: g_first(0, n),
        FIRST_VALUE: lambda n: g_first(1, n),
        BACK_QUERY: lambda n: back_query(),
        G_KEY: lambda n: g_step(0, n),
        OWN_KEY: lambda n: g_own(0),
        BACK_KEYS: lambda n: back_keys(),
        G_VALUE: lambda n: g_step(1, n),
        OWN_VALUE: lambda n: g_own(1),
        BACK_VALUES: lambda n: back_values(),
        INNER_GRAD: lambda n: inner_grad(),
        FINISH_BRANCH: lambda n: branch_end(),
    }
    for piece, (_, make, across, come, chain, end) in enumerate(PIECES):
        behind[make] = functools.partial(make_terms, piece)
        behind[across] = functools.partial(send_across, piece)
        behind[come] = functools.partial(gather_y, piece)
        behind[chain] = functools.partial(pass_z, piece)
        behind[end] = lambda n, piece=piece: finish(piece)
    for name, number in backward_steps(seq_count):
        behind[name](number)
    for piece in range(4):
        out_copy(piece).wait()
    branch_copy().wait()

    def left(ref, rows, sem):
        block = ref.at[:, pl.ds(0, rows), :]
        remote(block, block, sem, w_recv.at[0, 0], beside_device).wait_send()

    def drain():
        both, peers = seq_count * chip_count, seq_count * (chip_count - 1)
        if peers:
            left(weights, peers * own_rows, w_send.at[1])
            left(chip_in, peers * own_rows, t_send.at[1])
        left(weights, both * own_rows, w_send.at[2])
        left(held, both * own_rows, t_send.at[0])
        if seq_count > 1:
            left(chain_in, (seq_count - 1) * own_rows, t_send.at[2])
            left(part, (seq_count - 1) * token_count, g_send.at[0])

            @pl.when(at_end)
            def _():
                left(weights, own_rows, w_send.at[0])
                left(part_in, token_count, p_send.at[0])

            @pl.when(jnp.logical_not(at_end))
            def _():
                left(weights, (seq_count + 1) * own_rows, w_send.at[0])
                left(part_in, (seq_count + 1) * token_count, p_send.at[0])

        for step in range(1, tensor_count):
            x_copy(step).wait_send()
            xs_copy(step).wait_send()

    drain()


def local(tokens, cotangent, qkv_weight, out_weight):
    seq_count, dp_count = lax.axis_size("seq"), lax.axis_size("dp")
    tensor_count = lax.axis_size("tensor")
    chip_count = dp_count // CORES
    row_count, feature_count = tokens.shape[1:]
    own_rows, columns = out_weight.shape
    head_count = columns // HD
    share = feature_count // tensor_count
    sizes = (seq_count, dp_count, tensor_count, own_rows, head_count)

    def vmem(*shape, kind=BF16):
        return pltpu.VMEM(shape, kind)

    def dma(*shape):
        return pltpu.SemaphoreType.DMA(shape)

    both, peers = seq_count * chip_count, seq_count * max(chip_count - 1, 1)
    others = max(tensor_count - 1, 1)
    scratch = [
        vmem(row_count, feature_count),
        vmem(row_count, feature_count),
        vmem(row_count, feature_count),
        vmem(feature_count, row_count),
        vmem(feature_count, row_count),
        vmem(row_count, 128, kind=F32),
        vmem(row_count, 128, kind=F32),
        vmem(4, feature_count, columns),
        vmem(4, row_count, columns, kind=F32),
        vmem(2, seq_count * row_count, columns),
        vmem(row_count, columns),
        vmem(row_count, columns, kind=F32),
        vmem(row_count, columns, kind=F32),
        vmem(row_count, columns, kind=F32),
        vmem(row_count, columns, kind=F32),
        vmem(row_count, columns),
        vmem(head_count * seq_count * row_count, row_count),
        vmem(head_count, row_count, HD, kind=F32),
        vmem(head_count, row_count, HD, kind=F32),
        vmem(row_count, columns, kind=F32),
        vmem(row_count, columns),
        vmem(row_count, columns, kind=F32),
        vmem(2, seq_count * row_count, columns),
        vmem(2, (seq_count + 1) * row_count, columns),
        vmem(3, row_count, columns),
        vmem(tensor_count, row_count, share),
        vmem(others, row_count, share),
        vmem(2, row_count, 128, kind=F32),
        vmem(4, feature_count, columns),
        vmem(4, both * own_rows, columns),
        vmem(4, peers * own_rows, columns),
        vmem(4, (seq_count + 1) * own_rows, columns),
        vmem(4, own_rows, columns, kind=F32),
        vmem(row_count, share),
        vmem(8, row_count, kind=F32),
        vmem(others, 8, row_count, kind=F32),
        vmem(row_count, 8, kind=F32),
        dma(5),
        dma(5),
        dma(4, seq_count * dp_count),
        dma(3),
        dma(2, seq_count),
        dma(1),
        dma(2, seq_count),
        dma(2, seq_count),
        dma(1),
        dma(4, both),
        dma(4, peers),
        dma(3),
        dma(4, seq_count),
        dma(4, seq_count),
        dma(others),
        dma(others),
        dma(others),
        dma(others),
    ]
    anywhere = pl.BlockSpec(memory_space=pl.ANY)
    qkv_grad, out_grad, branch = pl.pallas_call(
        functools.partial(body, sizes),
        out_shape=(
            jax.ShapeDtypeStruct((3, own_rows, columns), F32),
            jax.ShapeDtypeStruct((own_rows, columns), F32),
            jax.ShapeDtypeStruct((row_count, share), BF16),
        ),
        in_specs=[anywhere] * 4,
        out_specs=(anywhere, anywhere, anywhere),
        scratch_shapes=scratch,
        compiler_params=pltpu.CompilerParams(
            collective_id=0, has_side_effects=True, vmem_limit_bytes=67043328
        ),
        name="layer",
    )(tokens[0], cotangent[0], jnp.transpose(qkv_weight, (1, 0, 2)), out_weight)
    return jnp.transpose(qkv_grad, (1, 0, 2)), out_grad, branch[None]


def solution(mesh):
    return jax.shard_map(
        local,
        mesh=mesh,
        in_specs=(
            P("dp", "seq", None),
            P("dp", "seq", None),
            P(("seq", "dp"), None, "tensor"),
            P(("seq", "dp"), "tensor"),
        ),
        out_specs=(
            P(("seq", "dp"), None, "tensor"),
            P(("seq", "dp"), "tensor"),
            P("dp", "seq", "tensor"),
        ),
        check_vma=False,
    )
```

```python
import functools

import jax
import jax.numpy as jnp
from jax import lax
from jax.experimental import pallas as pl
from jax.experimental.pallas import tpu as pltpu
from jax.sharding import PartitionSpec as P

HD = 128
CORES = 2
MESH_ID = pl.DeviceIdType.MESH
EPSILON = 1e-06
F32, BF16 = jnp.float32, jnp.bfloat16


(
    W_KV,
    OWN_QUERY,
    OWN_OUT,
    SPREAD_QUERY,
    SPREAD_OUT,
    CHIP_KV,
    MIX_KV,
    KEY_READY,
    W_QUERY,
    W_OUT,
    SEND_PAIRS,
    FLIP_UNIT,
    FLIP_COT,
    CHIP_QUERY,
    CHIP_OUT,
    MIX_QUERY,
    MIX_OUT,
    PAIR,
    QUERY_READY,
    LEND_QUERY,
    ATTEND,
    ATTEND_END,
    BORROW_QUERY,
    ATTEND_OTHER,
    GIVE_OUT,
    GRAD_READY,
    LEND_GRAD,
    BACKWARD,
    TAKE_OUT,
    BORROW_GRAD,
    BACKWARD_OTHER,
    FIRST_KEY,
    FIRST_VALUE,
    GIVE_QUERY,
    MAKE_OUT,
    ACROSS_OUT,
    BACK_QUERY,
    MAKE_QUERY,
    ACROSS_QUERY,
    Y_OUT,
    G_KEY,
    OWN_KEY,
    BACK_KEYS,
    MAKE_KEY,
    ACROSS_KEY,
    G_VALUE,
    OWN_VALUE,
    BACK_VALUES,
    MAKE_VALUE,
    ACROSS_VALUE,
    Y_QUERY,
    Z_OUT,
    INNER_GRAD,
    Y_KEY,
    Z_QUERY,
    Y_VALUE,
    Z_KEY,
    Z_VALUE,
    FINISH_OUT,
    FINISH_QUERY,
    FINISH_KEY,
    FINISH_BRANCH,
    FINISH_VALUE,
) = range(63)
FORWARD_TIMES = {
    W_KV: (0.41, 2.48),
    OWN_QUERY: (-35.12, 0.16),
    OWN_OUT: (-28.38, 1.52),
    SPREAD_QUERY: (7.47, 0.92),
    SPREAD_OUT: (-12.93, 0.0),
    CHIP_KV: (8.55, 3.24),
    MIX_KV: (-32.56, 4.81),
    KEY_READY: (5.33, 0.0),
    W_QUERY: (22.56, 4.24),
    W_OUT: (29.16, 3.65),
    SEND_PAIRS: (34.01, 2.08),
    FLIP_UNIT: (47.59, 3.24),
    FLIP_COT: (-1.26, 5.59),
    CHIP_QUERY: (36.68, 3.45),
    CHIP_OUT: (51.83, 3.22),
    MIX_QUERY: (53.59, 0.0),
    MIX_OUT: (78.74, 2.36),
    PAIR: (44.44, 1.99),
    QUERY_READY: (27.52, 0.84),
    LEND_QUERY: (8.55, 2.18),
    ATTEND: (-3.33, 3.06),
    ATTEND_END: (65.5, 0.0),
    BORROW_QUERY: (53.42, 0.97),
    ATTEND_OTHER: (33.53, 2.02),
    GIVE_OUT: (31.15, 0.3),
    GRAD_READY: (60.02, 0.25),
    LEND_GRAD: (28.36, 0.0),
}
BACKWARD_TIMES = {
    BACKWARD: (2.44, 0.88),
    TAKE_OUT: (-26.82, 0.0),
    BORROW_GRAD: (-12.76, 4.8),
    BACKWARD_OTHER: (-3.78, 1.86),
    FIRST_KEY: (-1.37, 1.7),
    FIRST_VALUE: (10.84, 4.04),
    GIVE_QUERY: (13.49, 1.36),
    MAKE_OUT: (-43.71, 2.7),
    ACROSS_OUT: (-1.45, 1.38),
    BACK_QUERY: (-0.89, 0.0),
    MAKE_QUERY: (8.55, 2.05),
    ACROSS_QUERY: (1.13, 0.0),
    Y_OUT: (10.77, 1.73),
    G_KEY: (13.06, 4.75),
    OWN_KEY: (-5.55, 0.0),
    BACK_KEYS: (25.83, 0.21),
    MAKE_KEY: (-0.38, 0.03),
    ACROSS_KEY: (23.41, 0.74),
    G_VALUE: (-2.95, 1.82),
    OWN_VALUE: (26.8, 0.0),
    BACK_VALUES: (9.31, 2.34),
    MAKE_VALUE: (31.42, 4.75),
    ACROSS_VALUE: (41.03, 0.54),
    Y_QUERY: (18.18, 7.26),
    Z_OUT: (27.24, 6.05),
    INNER_GRAD: (33.2, 0.0),
    Y_KEY: (39.48, 2.63),
    Z_QUERY: (29.97, 5.88),
    Y_VALUE: (50.93, 0.0),
    Z_KEY: (35.92, 6.83),
    Z_VALUE: (49.24, 5.92),
    FINISH_OUT: (40.19, 1.65),
    FINISH_QUERY: (51.68, 1.46),
    FINISH_KEY: (70.55, 1.91),
    FINISH_BRANCH: (78.24, 3.0),
    FINISH_VALUE: (123.85, 3.1),
}


PIECES = (
    (BACK_KEYS, MAKE_KEY, ACROSS_KEY, Y_KEY, Z_KEY, FINISH_KEY),
    (BACK_VALUES, MAKE_VALUE, ACROSS_VALUE, Y_VALUE, Z_VALUE, FINISH_VALUE),
    (BACK_QUERY, MAKE_QUERY, ACROSS_QUERY, Y_QUERY, Z_QUERY, FINISH_QUERY),
    (TAKE_OUT, MAKE_OUT, ACROSS_OUT, Y_OUT, Z_OUT, FINISH_OUT),
)


def events_until(k, seq_count):
    return min(2 * (seq_count - 1), 4 * ((k + 1) // 2))


def forward_steps(seq_count):
    events, needs = 2 * (seq_count - 1), {}

    def chained(name, count, more):
        for n in range(count):
            needs[name, n] = ([(name, n - 1)] if n else []) + more(n)

    chained(W_KV, events, lambda n: [])
    chained(CHIP_KV, events + 2, lambda n: [(W_KV, n - 2)] if n > 1 else [])
    chained(MIX_KV, seq_count, lambda k: [(CHIP_KV, 1 + events_until(k, seq_count))])
    streams = (
        (OWN_QUERY, SPREAD_QUERY, W_QUERY, CHIP_QUERY, MIX_QUERY),
        (OWN_OUT, SPREAD_OUT, W_OUT, CHIP_OUT, MIX_OUT),
    )
    for own, spread, come, across, mix in streams:
        needs[own, 0] = [(W_KV, min(4, events) - 1)]
        needs[own, 1] = [(own, 0), (W_KV, events - 1)]
        needs[spread, 0] = [(own, 1)]
        chained(come, seq_count - 1, lambda n: [(own, 1)])
        chained(across, seq_count, lambda n: [(come, n - 1)] if n else [(spread, 0)])
        chained(mix, seq_count, lambda n: [(across, n)])
    needs[W_OUT, 0].append((W_QUERY, seq_count - 2))
    needs[SPREAD_OUT, 0].append((W_QUERY, seq_count - 2))
    needs[CHIP_OUT, 0].append((CHIP_QUERY, seq_count - 1))
    needs[KEY_READY, 0] = [(MIX_KV, seq_count - 1)]
    needs[SEND_PAIRS, 0] = [(KEY_READY, 0)]
    needs[FLIP_UNIT, 0] = needs[FLIP_COT, 0] = []
    chained(PAIR, events, lambda n: [(SEND_PAIRS, 0)])
    needs[QUERY_READY, 0] = [(MIX_QUERY, seq_count - 1)]
    needs[LEND_QUERY, 0] = [(QUERY_READY, 0)]
    needs[BORROW_QUERY, 0] = [(LEND_QUERY, 0)]

    def there(k):
        until = events_until(k, seq_count)
        return [(KEY_READY, 0)] + ([(PAIR, until - 1)] if until else [])

    chained(ATTEND, seq_count, lambda k: [(QUERY_READY, 0)] + there(k))
    chained(ATTEND_OTHER, seq_count, lambda k: [(BORROW_QUERY, 0)] + there(k))
    needs[ATTEND_END, 0] = [(ATTEND, seq_count - 1)]
    needs[GIVE_OUT, 0] = [(ATTEND_OTHER, seq_count - 1)]
    needs[GRAD_READY, 0] = [(MIX_OUT, seq_count - 1)]
    needs[LEND_GRAD, 0] = [(GRAD_READY, 0)]
    return in_order(needs, FORWARD_TIMES)


def backward_steps(seq_count):
    needs, last = {}, seq_count - 1

    def chained(name, count, more):
        for n in range(count):
            needs[name, n] = ([(name, n - 1)] if n else []) + more(n)

    chained(BACKWARD, seq_count, lambda n: [])
    for first, come, own in ((FIRST_KEY, G_KEY, OWN_KEY), (FIRST_VALUE, G_VALUE, OWN_VALUE)):
        chained(first, seq_count, lambda n: [(BACKWARD_OTHER, n)])
        chained(come, last, lambda n: [(first, last)])
        needs[own, 0] = [(come, last - 1) if last else (first, last)]
    needs[BORROW_GRAD, 0] = needs[TAKE_OUT, 0] = []
    chained(BACKWARD_OTHER, seq_count, lambda n: [(BACKWARD, n), (BORROW_GRAD, 0)])
    needs[GIVE_QUERY, 0] = [(BACKWARD_OTHER, last)]
    needs[BACK_QUERY, 0] = [(BACKWARD, last), (GIVE_QUERY, 0)]
    needs[BACK_KEYS, 0] = [(OWN_KEY, 0)]
    needs[BACK_VALUES, 0] = [(OWN_VALUE, 0)]
    for ready, make, across, come, chain, finish in PIECES:
        first = [(ready, 0)]
        chained(make, seq_count, lambda n: first)
        chained(across, seq_count, lambda n: [(make, n)])
        chained(come, seq_count, lambda n: [(across, n)])
        chained(chain, last, lambda n: [(come, n)])
        needs[finish, 0] = [(come, last)] + ([(chain, last - 1)] if last else [])
    needs[INNER_GRAD, 0] = [(BACK_VALUES, 0), (BACK_KEYS, 0), (BACK_QUERY, 0)]
    needs[FINISH_BRANCH, 0] = [(INNER_GRAD, 0)]
    return in_order(needs, BACKWARD_TIMES)


def in_order(needs, times):
    left, steps = dict(needs), []
    while left:
        able = [step for step in left if not any(other in left for other in left[step])]
        best = min(able, key=lambda step: (times[step[0]][0] + times[step[0]][1] * step[1], step))
        steps.append(best)
        del left[best]
    return steps


def dot(left, right):
    return jnp.dot(left, right, preferred_element_type=F32)


def dot_nt(left, right):
    return lax.dot_general(left, right, (((1,), (1,)), ((), ())), preferred_element_type=F32)


def dot_tn(left, right):
    return lax.dot_general(left, right, (((0,), (0,)), ((), ())), preferred_element_type=F32)


def normalize(values):
    centered = values - jnp.mean(values, axis=-1, keepdims=True)
    inverse = lax.rsqrt(jnp.mean(centered * centered, axis=-1, keepdims=True) + EPSILON)
    return centered * inverse, inverse


def normalize_back(gradient, normed, inverse):
    mean_grad = jnp.mean(gradient, axis=-1, keepdims=True)
    mean_both = jnp.mean(gradient * normed, axis=-1, keepdims=True)
    return (gradient - mean_grad - normed * mean_both) * inverse


def body(
    sizes,
    tokens_hbm,
    cotangent_hbm,
    qkv_hbm,
    outw_hbm,
    qkv_out,
    outw_out,
    branch_hbm,
    tok,
    cot,
    unit_low,
    unit_t,
    cot_t,
    stat_mean,
    stat_inv,
    weights,
    acc,
    pairs,
    query_low,
    query_unit,
    key_unit,
    query_inv,
    key_inv,
    grad_low,
    query_out,
    query_in,
    expo,
    totals,
    deltas,
    weighted,
    attended,
    query_raw,
    part,
    part_in,
    back,
    inner,
    inner_in,
    sums,
    terms,
    held,
    chip_in,
    chain_in,
    summed,
    branch_out,
    sum_rows,
    sum_rows_in,
    sum_columns,
    load_sem,
    store_sem,
    w_recv,
    w_send,
    p_recv,
    p_send,
    g_low,
    g_high,
    g_send,
    h_send,
    h_recv,
    t_core_recv,
    t_chip_recv,
    t_send,
    t_low_recv,
    t_high_recv,
    x_send,
    x_recv,
    xs_send,
    xs_recv,
):
    seq_count, dp_count, tensor_count, own_rows, head_count = sizes
    chip_count = dp_count // CORES
    token_count, feature_count = tok.shape
    share = feature_count // tensor_count
    plane = dp_count * own_rows
    scale = HD ** (-0.5)
    place = lax.axis_index("seq")
    index = lax.axis_index("dp")
    lane = lax.axis_index("tensor")
    chip, core = index // CORES, index % CORES
    not_last, not_first = place < seq_count - 1, place > 0
    both_sides = jnp.minimum(place, seq_count - 1 - place)
    at_end = both_sides == 0
    inside = both_sides > 0
    helps = both_sides == 1
    can_right, can_left = place < seq_count - 2, place > 1
    KEY, VALUE, QUERY, OUT = range(4)

    def rows_of(slot):
        return pl.ds(pl.multiple_of(slot * own_rows, own_rows), own_rows)

    def block_rows(origin):
        return pl.ds(pl.multiple_of(origin * token_count, token_count), token_count)

    own_rows_at = rows_of(place * dp_count + index)
    loads = [
        pltpu.make_async_copy(
            qkv_hbm.at[pl.ds(1, 2)], weights.at[pl.ds(0, 2), own_rows_at, :], load_sem.at[0]
        ),
        pltpu.make_async_copy(qkv_hbm.at[0], weights.at[QUERY, own_rows_at, :], load_sem.at[1]),
        pltpu.make_async_copy(outw_hbm, weights.at[OUT, own_rows_at, :], load_sem.at[2]),
        pltpu.make_async_copy(tokens_hbm, tok, load_sem.at[3]),
        pltpu.make_async_copy(cotangent_hbm, cot, load_sem.at[4]),
    ]
    for load in loads:
        load.start()

    barrier = pltpu.get_barrier_semaphore()

    def signal(device):
        pl.semaphore_signal(barrier, inc=1, device_id=device, device_id_type=MESH_ID)

    def greet():
        @pl.when(not_first)
        def _():
            signal({"seq": place - 1})

        @pl.when(not_last)
        def _():
            signal({"seq": place + 1})

        for step in range(1, chip_count):
            signal({"dp": (chip + step) % chip_count * CORES + core})
        signal({"dp": chip * CORES + 1 - core})
        for step in range(1, tensor_count):
            signal({"tensor": (lane + step) % tensor_count})
        ends = jnp.minimum(place, 1) + jnp.minimum(seq_count - 1 - place, 1)
        pl.semaphore_wait(barrier, chip_count + tensor_count - 1 + ends)

    greet()

    def remote(source, target, send_sem, recv_sem, device):
        return pltpu.make_async_remote_copy(
            src_ref=source,
            dst_ref=target,
            send_sem=send_sem,
            recv_sem=recv_sem,
            device_id=device,
            device_id_type=MESH_ID,
        )

    up, down = {"seq": place + 1}, {"seq": place - 1}
    beside_device = {"dp": chip * CORES + 1 - core}

    def chip_device(step):
        return {"dp": (chip + step) % chip_count * CORES + core}

    def origin_at(k):
        near = jnp.where(k % 2 == 1, place - (k + 1) // 2, place + k // 2)
        far = jnp.where(
            place * 2 > seq_count - 1, place - (k - both_sides), place + (k - both_sides)
        )
        return jnp.where(k <= 2 * both_sides, near, far)

    def event(number):
        group, rest = number // 4, number % 4
        if 2 * group + 2 <= seq_count - 1:
            paired = both_sides > group
            piece = jnp.where(paired, rest // 2, rest % 2)
            k = 2 * group + 1 + jnp.where(paired, rest % 2, rest // 2)
        else:
            piece, k = rest % 2, 2 * group + 1 + rest // 2
        return piece, origin_at(k)

    def w_copy(piece, slot, send_sem, device, source=None):
        ref = weights.at[piece, rows_of(slot), :]
        return remote(ref if source is None else source, ref, send_sem, w_recv.at[piece, slot], device)

    def w_side(piece, origin, rightward, source=None):
        if rightward:
            return w_copy(piece, origin * dp_count + index, w_send.at[0], up, source)
        return w_copy(piece, origin * dp_count + index, w_send.at[0], down, source)

    def w_across(piece, origin, step, source=None):
        return w_copy(piece, origin * dp_count + index, w_send.at[1], chip_device(step), source)

    def w_beside(piece, origin, source_chip, source=None):
        slot = origin * dp_count + source_chip * CORES + core
        return w_copy(piece, slot, w_send.at[2], beside_device, source)

    def w_landed(piece, slot):
        w_copy(piece, slot, w_send.at[2], beside_device).wait_recv()

    def w_sides_own(piece, source=None):
        @pl.when(not_last)
        def _():
            w_side(piece, place, True, source).start()

        @pl.when(not_first)
        def _():
            w_side(piece, place, False, source).start()

    def w_spread_own(piece, source=None):
        for step in range(1, chip_count):
            w_across(piece, place, step, source).start()
        w_beside(piece, place, chip, source).start()

    def w_step(piece, origin):
        w_landed(piece, origin * dp_count + index)

        @pl.when((origin < place) & not_last)
        def _():
            w_side(piece, origin, True).start()

        @pl.when((origin > place) & not_first)
        def _():
            w_side(piece, origin, False).start()

        for step in range(1, chip_count):
            w_across(piece, origin, step).start()
        w_beside(piece, origin, chip).start()

    def w_chip_step(piece, origin):
        for step in range(1, chip_count):
            source_chip = (chip + step) % chip_count
            w_landed(piece, origin * dp_count + source_chip * CORES + core)
            w_beside(piece, origin, source_chip).start()

    def project(piece, k):
        origin = origin_at(k)
        rows = pl.ds(pl.multiple_of(origin * plane, plane), plane)
        for source_chip in range(chip_count):
            w_landed(piece, origin * dp_count + source_chip * CORES + 1 - core)
        source = cot if piece == OUT else unit_low
        product = dot(source[:, rows], weights[piece, rows, :])
        if k == 0:
            acc[piece] = product
        else:
            acc[piece] += product

    def p_copy(piece, origin, rightward):
        ref = pairs.at[piece, block_rows(origin), :]
        if rightward:
            return remote(ref, ref, p_send.at[0], p_recv.at[piece, origin], up)
        return remote(ref, ref, p_send.at[0], p_recv.at[piece, origin], down)

    def p_step(number):
        piece, origin = event(number)

        @pl.when(inside)
        def _():
            p_copy(piece, origin, True).wait_recv()

            @pl.when((origin < place) & can_right)
            def _():
                p_copy(piece, origin, True).start()

            @pl.when((origin > place) & can_left)
            def _():
                p_copy(piece, origin, False).start()

    def p_sides_own():
        for piece in range(2):

            @pl.when(can_right)
            def _():
                p_copy(piece, place, True).start()

            @pl.when(can_left)
            def _():
                p_copy(piece, place, False).start()

    def loan(source, target, number, device):
        return remote(source, target, h_send.at[number], h_recv.at[number], device)

    def lend(source, target, number):
        @pl.when(place == 0)
        def _():
            loan(source, target, number, up).start()

        @pl.when(place == seq_count - 1)
        def _():
            loan(source, target, number, down).start()

    def give(source, target, number):
        @pl.when(place == 1)
        def _():
            loan(source, target, number, down).start()

        @pl.when(place == seq_count - 2)
        def _():
            loan(source, target, number, up).start()

    def loans():
        return (
            (query_low.at[0], query_low.at[1]),
            (grad_low.at[0], grad_low.at[1]),
            (attended.at[1], attended.at[0]),
            (query_out, query_in),
        )

    def loan_wait(number):
        source, target = loans()[number]
        loan(source, target, number, up).wait_recv()

    def normalize_tokens():
        @pl.loop(0, token_count // 32)
        def _(step):
            rows = pl.ds(pl.multiple_of(step * 32, 32), 32)
            values = tok[rows, :].astype(F32)
            average = jnp.mean(values, axis=-1, keepdims=True)
            centered = values - average
            inverse = lax.rsqrt(jnp.mean(centered * centered, axis=-1, keepdims=True) + EPSILON)
            unit_low[rows, :] = (centered * inverse).astype(BF16)
            stat_mean[rows, :] = jnp.broadcast_to(average, (32, 128))
            stat_inv[rows, :] = jnp.broadcast_to(inverse, (32, 128))

    def flip(source, target):
        @pl.loop(0, feature_count // 128)
        def _(step):
            cut = pl.ds(pl.multiple_of(step * 128, 128), 128)
            target[cut, :] = source[:, cut].T

    def key_ready():
        own_block = block_rows(place)
        for h in range(head_count):
            cut = slice(h * HD, (h + 1) * HD)
            normed, inverse = normalize(acc[KEY, :, cut])
            key_unit[:, cut] = normed
            key_inv[:, cut] = jnp.broadcast_to(inverse, (token_count, HD))
            pairs[0, own_block, cut] = normed.astype(BF16)
            pairs[1, own_block, cut] = acc[VALUE, :, cut].astype(BF16)

    def query_ready():
        for h in range(head_count):
            cut = slice(h * HD, (h + 1) * HD)
            normed, inverse = normalize(acc[QUERY, :, cut])
            query_unit[:, cut] = normed
            query_inv[:, cut] = jnp.broadcast_to(inverse, (token_count, HD))
            query_low[0, :, cut] = normed.astype(BF16)

    def grad_ready():
        grad_low[0] = acc[OUT].astype(BF16)

    for piece in (KEY, VALUE):
        w_sides_own(piece, qkv_hbm.at[1 + piece])
    for piece in (KEY, VALUE):
        w_spread_own(piece, qkv_hbm.at[1 + piece])
    for load in loads:
        load.wait()
    normalize_tokens()

    def expo_at(who, origin, h):
        row = ((who * head_count + h) * seq_count + origin) * token_count
        return pl.ds(pl.multiple_of(row, token_count), token_count)

    def attend_rows(who, k):
        origin = origin_at(k)
        rows = block_rows(origin)
        for h in range(head_count):
            cut = slice(h * HD, (h + 1) * HD)
            scores = dot_nt(query_low[who, :, cut], pairs[0, rows, cut]) * scale
            exponent = jnp.exp(scores)
            low = exponent.astype(BF16)
            expo[expo_at(who, origin, h), :] = low
            total = exponent[:, :HD]
            for at in range(HD, token_count, HD):
                total = total + exponent[:, at : at + HD]
            mixed = dot(low, pairs[1, rows, cut])
            if k == 0:
                totals[who * head_count + h] = total
                weighted[who, :, cut] = mixed
            else:
                totals[who * head_count + h] += total
                weighted[who, :, cut] += mixed

    def attend(k):
        pl.when(inside)(lambda: attend_rows(0, k))

    def attend_other(k):
        pl.when(helps)(lambda: attend_rows(1, k))

    def attend_end(who):
        for h in range(head_count):
            cut = slice(h * HD, (h + 1) * HD)
            total = jnp.sum(totals[who * head_count + h], axis=-1, keepdims=True)
            attended[who, :, cut] = (weighted[who, :, cut] / total).astype(BF16)
            totals[who * head_count + h] = jnp.broadcast_to(1.0 / total, (token_count, HD))

    def attend_delta(who):
        for h in range(head_count):
            cut = slice(h * HD, (h + 1) * HD)
            both = grad_low[who, :, cut].astype(F32) * attended[who, :, cut].astype(F32)
            delta = jnp.sum(both, axis=-1, keepdims=True)
            deltas[who * head_count + h] = jnp.broadcast_to(delta, (token_count, HD))

    def own_stream(piece, number):
        @pl.when(inside if number else at_end)
        def _():
            w_sides_own(piece)

    def kv_step(number):
        piece, origin = event(number)
        w_step(piece, origin)

    def kv_chip(number):
        piece, origin = (number, place) if number < 2 else event(number - 2)
        w_chip_step(piece, origin)

    def kv_mix(k):
        project(KEY, k)
        project(VALUE, k)

    def give_out():
        @pl.when(helps)
        def _():
            attend_end(1)
            give(*loans()[2], 2)

    ahead = {
        W_KV: kv_step,
        OWN_QUERY: lambda n: own_stream(QUERY, n),
        OWN_OUT: lambda n: own_stream(OUT, n),
        SPREAD_QUERY: lambda n: w_spread_own(QUERY),
        SPREAD_OUT: lambda n: w_spread_own(OUT),
        CHIP_KV: kv_chip,
        MIX_KV: kv_mix,
        KEY_READY: lambda n: key_ready(),
        W_QUERY: lambda n: w_step(QUERY, origin_at(n + 1)),
        W_OUT: lambda n: w_step(OUT, origin_at(n + 1)),
        CHIP_QUERY: lambda n: w_chip_step(QUERY, origin_at(n)),
        CHIP_OUT: lambda n: w_chip_step(OUT, origin_at(n)),
        MIX_QUERY: lambda n: project(QUERY, n),
        MIX_OUT: lambda n: project(OUT, n),
        SEND_PAIRS: lambda n: p_sides_own(),
        FLIP_UNIT: lambda n: flip(unit_low, unit_t),
        FLIP_COT: lambda n: flip(cot, cot_t),
        PAIR: p_step,
        QUERY_READY: lambda n: query_ready(),
        LEND_QUERY: lambda n: lend(*loans()[0], 0),
        BORROW_QUERY: lambda n: pl.when(helps)(lambda: loan_wait(0)),
        ATTEND: attend,
        ATTEND_OTHER: attend_other,
        ATTEND_END: lambda n: pl.when(inside)(lambda: attend_end(0)),
        GIVE_OUT: lambda n: give_out(),
        GRAD_READY: lambda n: grad_ready(),
        LEND_GRAD: lambda n: lend(*loans()[1], 1),
    }
    for name, number in forward_steps(seq_count):
        ahead[name](number)

    pl.when(inside)(lambda: attend_delta(0))

    def target_at(n):
        return origin_at(seq_count - 1 - n)

    def from_above(target, receiver):
        return jnp.where(target == receiver, seq_count, target)

    def add_into(ref, piece, slot, others, size):
        @pl.loop(0, size // 16)
        def _(step):
            def cut(at):
                return pl.ds(pl.multiple_of(at * size + step * 16, 16), 16)

            total = ref[piece, cut(slot), :].astype(F32)
            for other, at in others:
                total = total + other[piece, cut(at), :].astype(F32)
            ref[piece, cut(slot), :] = total.astype(BF16)

    def g_copy(piece, target, rightward):
        rows = block_rows(target)
        source = part.at[piece, rows, :]
        if rightward:
            into, sem, device = rows, g_low, up
        else:
            into, sem, device = block_rows(from_above(target, place - 1)), g_high, down
        into = part_in.at[piece, into, :]
        return remote(source, into, g_send.at[0], sem.at[piece, target], device)

    def backward_rows(who, n):
        target = target_at(n)
        rows = block_rows(target)
        for h in range(head_count):
            cut = slice(h * HD, (h + 1) * HD)
            inv_total = totals[who * head_count + h][:, :1]
            probability = expo[expo_at(who, target, h), :].astype(F32) * inv_total
            gradient = grad_low[who, :, cut]
            prob_grad = dot_nt(gradient, pairs[1, rows, cut])
            delta = deltas[who * head_count + h][:, :1]
            score = (probability * (prob_grad - delta) * scale).astype(BF16)
            query_part = dot(score, pairs[0, rows, cut])
            key_part = dot_tn(score, query_low[who, :, cut])
            value_part = dot_tn(probability.astype(BF16), gradient)
            if who:
                key_part = key_part + part[0, rows, cut].astype(F32)
                value_part = value_part + part[1, rows, cut].astype(F32)
            part[0, rows, cut] = key_part.astype(BF16)
            part[1, rows, cut] = value_part.astype(BF16)
            if n == 0:
                query_raw[who, :, cut] = query_part
            else:
                query_raw[who, :, cut] += query_part

    def backward(n):
        pl.when(inside)(lambda: backward_rows(0, n))

    def backward_other(n):
        pl.when(helps)(lambda: backward_rows(1, n))

    def borrow_grad():
        @pl.when(helps)
        def _():
            loan_wait(1)
            attend_delta(1)

    def give_query():
        @pl.when(helps)
        def _():
            query_out[...] = query_raw[1].astype(BF16)
            give(*loans()[3], 3)

    def g_first(piece, n):
        target = target_at(n)

        @pl.when((target > place) & (place == 1))
        def _():
            g_copy(piece, target, True).start()

        @pl.when((target < place) & (place == seq_count - 2))
        def _():
            g_copy(piece, target, False).start()

    def g_step(piece, n):
        target = target_at(n)

        @pl.when((place < target) & inside & can_left)
        def _():
            g_copy(piece, target, True).wait_recv()
            add_into(part, piece, target, [(part_in, target)], token_count)
            g_copy(piece, target, True).start()

        @pl.when((place > target) & inside & can_right)
        def _():
            g_copy(piece, target, False).wait_recv()
            add_into(part, piece, target, [(part_in, target)], token_count)
            g_copy(piece, target, False).start()

    def g_own(piece):
        own = block_rows(place)

        @pl.when(at_end)
        def _():
            part[piece, own, :] = jnp.zeros((token_count, head_count * HD), BF16)

        @pl.when(can_left)
        def _():
            g_copy(piece, place, True).wait_recv()
            add_into(part, piece, place, [(part_in, place)], token_count)

        @pl.when(can_right)
        def _():
            g_copy(piece, place, False).wait_recv()
            add_into(part, piece, place, [(part_in, seq_count)], token_count)

    def back_query():
        @pl.when(at_end)
        def _():
            loan_wait(3)
            query_raw[0] = query_in[...].astype(F32)

        for h in range(head_count):
            cut = slice(h * HD, (h + 1) * HD)
            raised = normalize_back(query_raw[0, :, cut], query_unit[:, cut], query_inv[:, cut])
            back[QUERY, :, cut] = raised.astype(BF16)

    def back_keys():
        own_block = block_rows(place)
        for h in range(head_count):
            cut = slice(h * HD, (h + 1) * HD)
            raw = part[0, own_block, cut].astype(F32)
            raised = normalize_back(raw, key_unit[:, cut], key_inv[:, cut])
            back[KEY, :, cut] = raised.astype(BF16)

    def back_values():
        back[VALUE] = part[1, block_rows(place), :]

    def t_beside(piece, target, target_chip):
        slot = target * chip_count + target_chip
        source = terms.at[piece, rows_of(target * dp_count + target_chip * CORES + 1 - core), :]
        into = held.at[piece, rows_of(slot), :]
        sems = t_send.at[0], t_core_recv.at[piece, slot]
        return remote(source, into, *sems, beside_device)

    def t_across(piece, target, step):
        other = (chip + step) % chip_count
        slot = (step - 1) * seq_count + target
        source = held.at[piece, rows_of(target * chip_count + other), :]
        into = chip_in.at[piece, rows_of(slot), :]
        sems = t_send.at[1], t_chip_recv.at[piece, slot]
        return remote(source, into, *sems, chip_device(step))

    def t_chain(piece, target, rightward):
        source = held.at[piece, rows_of(target * chip_count + chip), :]
        if rightward:
            at, sem, device = target, t_low_recv, up
        else:
            at, sem, device = from_above(target, place - 1), t_high_recv, down
        into = chain_in.at[piece, rows_of(at), :]
        return remote(source, into, t_send.at[2], sem.at[piece, target], device)

    def make_terms(piece, n):
        target = target_at(n)
        source = cot_t if piece == OUT else unit_t

        right = attended[0] if piece == OUT else back[piece]
        size = plane // CORES
        for at in range(CORES):
            rows = pl.ds(pl.multiple_of(target * plane + at * size, size), size)
            terms[piece, rows, :] = dot(source[rows, :], right).astype(BF16)

        for step in range(1, chip_count):
            t_beside(piece, target, (chip + step) % chip_count).start()
        t_beside(piece, target, chip).start()

    def send_across(piece, n):
        target = target_at(n)
        for step in range(1, chip_count):
            other = (chip + step) % chip_count
            t_beside(piece, target, other).wait_recv()
            own = target * dp_count + other * CORES + core
            add_into(held, piece, target * chip_count + other, [(terms, own)], own_rows)
            t_across(piece, target, step).start()

    def gather_y(piece, n):
        target = target_at(n)
        t_beside(piece, target, chip).wait_recv()
        others = [(terms, target * dp_count + index)]
        for step in range(1, chip_count):
            t_across(piece, target, step).wait_recv()
            others.append((chip_in, (step - 1) * seq_count + target))
        add_into(held, piece, target * chip_count + chip, others, own_rows)

        @pl.when((target > place) & (place == 0))
        def _():
            t_chain(piece, target, True).start()

        @pl.when((target < place) & (place == seq_count - 1))
        def _():
            t_chain(piece, target, False).start()

    def pass_z(piece, n):
        target = target_at(n)
        slot = target * chip_count + chip

        @pl.when((place < target) & not_first)
        def _():
            t_chain(piece, target, True).wait_recv()
            add_into(held, piece, slot, [(chain_in, target)], own_rows)
            t_chain(piece, target, True).start()

        @pl.when((place > target) & not_last)
        def _():
            t_chain(piece, target, False).wait_recv()
            add_into(held, piece, slot, [(chain_in, target)], own_rows)
            t_chain(piece, target, False).start()

    width = next(size for size in (512, 384, 256, 128) if share % size == 0)

    def lanes(values):
        total = values[:, :128]
        for at in range(128, width, 128):
            total = total + values[:, at : at + 128]
        return total

    def x_copy(step):
        other = (lane + step) % tensor_count
        sems = x_send.at[step - 1], x_recv.at[step - 1]
        return remote(inner.at[other], inner_in.at[step - 1], *sems, {"tensor": other})

    def xs_copy(step):
        other = (lane + step) % tensor_count
        sems = xs_send.at[step - 1], xs_recv.at[step - 1]
        return remote(sum_rows, sum_rows_in.at[step - 1], *sems, {"tensor": other})

    def inner_grad():
        sums[...] = jnp.zeros_like(sums)

        def tile(owner, step):
            start = owner * share + step * width
            cut = pl.ds(pl.multiple_of(start, width), width)
            product = dot_nt(back[QUERY], weights[QUERY, cut, :])
            product = product + dot_nt(back[KEY], weights[KEY, cut, :])
            product = product + dot_nt(back[VALUE], weights[VALUE, cut, :])
            unit = (tok[:, cut].astype(F32) - stat_mean[:, :1]) * stat_inv[:, :1]
            sums[0] += lanes(product)
            sums[1] += lanes(product * unit)
            at = pl.ds(pl.multiple_of(step * width, width), width)
            inner[owner, :, at] = product.astype(BF16)

        for turn in range(1, tensor_count + 1):

            @pl.loop(0, share // width)
            def _(step):
                tile((lane + turn) % tensor_count, step)

            if turn < tensor_count:
                x_copy(turn).start()
        sum_rows[...] = jnp.zeros_like(sum_rows)
        for at in range(2):
            sum_rows[at : at + 1, :] = jnp.sum(sums[at].T, axis=0, keepdims=True)
        for step in range(1, tensor_count):
            xs_copy(step).start()

    def finish_branch():
        for step in range(1, tensor_count):
            x_copy(step).wait_recv()
            xs_copy(step).wait_recv()
        total = sum_rows[...]
        for other in range(tensor_count - 1):
            total = total + sum_rows_in[other]
        sum_columns[...] = total.T / feature_count

        @pl.loop(0, token_count // 16)
        def _(step):
            rows = pl.ds(pl.multiple_of(step * 16, 16), 16)
            values = inner[lane, rows, :].astype(F32)
            for other in range(tensor_count - 1):
                values = values + inner_in[other, rows, :].astype(F32)
            means = sum_columns[rows, :]
            mean_grad, mean_both = means[:, 0:1], means[:, 1:2]
            cut = pl.ds(pl.multiple_of(lane * share, share), share)
            inverse = stat_inv[rows, :][:, :1]
            unit = (tok[rows, cut].astype(F32) - stat_mean[rows, :][:, :1]) * inverse
            branch_out[rows, :] = ((values - mean_grad - unit * mean_both) * inverse).astype(BF16)

    def finish_weights(piece):
        own_held = place * chip_count + chip

        @pl.when(not_first)
        def _():
            t_chain(piece, place, True).wait_recv()

        @pl.when(not_last)
        def _():
            t_chain(piece, place, False).wait_recv()

        @pl.loop(0, own_rows // 16)
        def _(step):
            rows = pl.ds(pl.multiple_of(step * 16, 16), 16)

            def cut(at):
                return pl.ds(pl.multiple_of(at * own_rows + step * 16, 16), 16)

            summed[piece, rows, :] = held[piece, cut(own_held), :].astype(F32)

            @pl.when(not_first)
            def _():
                summed[piece, rows, :] += chain_in[piece, cut(place), :].astype(F32)

            @pl.when(not_last)
            def _():
                summed[piece, rows, :] += chain_in[piece, cut(seq_count), :].astype(F32)

    def out_copy(piece):
        target = outw_out if piece == OUT else qkv_out.at[(1, 2, 0)[piece]]
        return pltpu.make_async_copy(summed.at[piece], target, store_sem.at[piece])

    def branch_copy():
        return pltpu.make_async_copy(branch_out, branch_hbm, store_sem.at[4])

    def finish(piece):
        finish_weights(piece)
        out_copy(piece).start()

    def branch_end():
        finish_branch()
        branch_copy().start()

    behind = {
        BACKWARD: backward,
        TAKE_OUT: lambda n: pl.when(at_end)(lambda: loan_wait(2)),
        BORROW_GRAD: lambda n: borrow_grad(),
        BACKWARD_OTHER: backward_other,
        GIVE_QUERY: lambda n: give_query(),
        FIRST_KEY: lambda n: g_first(0, n),
        FIRST_VALUE: lambda n: g_first(1, n),
        BACK_QUERY: lambda n: back_query(),
        G_KEY: lambda n: g_step(0, n),
        OWN_KEY: lambda n: g_own(0),
        BACK_KEYS: lambda n: back_keys(),
        G_VALUE: lambda n: g_step(1, n),
        OWN_VALUE: lambda n: g_own(1),
        BACK_VALUES: lambda n: back_values(),
        INNER_GRAD: lambda n: inner_grad(),
        FINISH_BRANCH: lambda n: branch_end(),
    }
    for piece, (_, make, across, come, chain, end) in enumerate(PIECES):
        behind[make] = functools.partial(make_terms, piece)
        behind[across] = functools.partial(send_across, piece)
        behind[come] = functools.partial(gather_y, piece)
        behind[chain] = functools.partial(pass_z, piece)
        behind[end] = lambda n, piece=piece: finish(piece)
    for name, number in backward_steps(seq_count):
        behind[name](number)
    for piece in range(4):
        out_copy(piece).wait()
    branch_copy().wait()

    def left(ref, rows, sem):
        block = ref.at[:, pl.ds(0, rows), :]
        remote(block, block, sem, w_recv.at[0, 0], beside_device).wait_send()

    def drain():
        both, peers = seq_count * chip_count, seq_count * (chip_count - 1)
        if peers:
            left(weights, peers * own_rows, w_send.at[1])
            left(chip_in, peers * own_rows, t_send.at[1])
        left(weights, both * own_rows, w_send.at[2])
        left(held, both * own_rows, t_send.at[0])
        if seq_count > 1:
            left(chain_in, (seq_count - 1) * own_rows, t_send.at[2])

            @pl.when(at_end)
            def _():
                left(weights, own_rows, w_send.at[0])
                left(part_in, token_count, p_send.at[0])
                for number in (0, 1):
                    loan(*loans()[number], number, up).wait_send()

            @pl.when(inside)
            def _():
                left(weights, (seq_count + 1) * own_rows, w_send.at[0])
                left(part, (seq_count - 1) * token_count, g_send.at[0])

            @pl.when(helps)
            def _():
                left(part_in, 2 * token_count, p_send.at[0])
                for number in (2, 3):
                    loan(*loans()[number], number, up).wait_send()

            @pl.when(both_sides > 1)
            def _():
                left(part_in, (seq_count + 1) * token_count, p_send.at[0])

        for step in range(1, tensor_count):
            x_copy(step).wait_send()
            xs_copy(step).wait_send()

    drain()


def local(tokens, cotangent, qkv_weight, out_weight):
    seq_count, dp_count = lax.axis_size("seq"), lax.axis_size("dp")
    tensor_count = lax.axis_size("tensor")
    chip_count = dp_count // CORES
    row_count, feature_count = tokens.shape[1:]
    own_rows, columns = out_weight.shape
    head_count = columns // HD
    share = feature_count // tensor_count
    assert seq_count > 3
    sizes = (seq_count, dp_count, tensor_count, own_rows, head_count)

    def vmem(*shape, kind=BF16):
        return pltpu.VMEM(shape, kind)

    def dma(*shape):
        return pltpu.SemaphoreType.DMA(shape)

    both, peers = seq_count * chip_count, seq_count * max(chip_count - 1, 1)
    others = max(tensor_count - 1, 1)
    scratch = [
        vmem(row_count, feature_count),
        vmem(row_count, feature_count),
        vmem(row_count, feature_count),
        vmem(feature_count, row_count),
        vmem(feature_count, row_count),
        vmem(row_count, 128, kind=F32),
        vmem(row_count, 128, kind=F32),
        vmem(4, feature_count, columns),
        vmem(4, row_count, columns, kind=F32),
        vmem(2, seq_count * row_count, columns),
        vmem(2, row_count, columns),
        vmem(row_count, columns, kind=F32),
        vmem(row_count, columns, kind=F32),
        vmem(row_count, columns, kind=F32),
        vmem(row_count, columns, kind=F32),
        vmem(2, row_count, columns),
        vmem(row_count, columns),
        vmem(row_count, columns),
        vmem(2 * head_count * seq_count * row_count, row_count),
        vmem(2 * head_count, row_count, HD, kind=F32),
        vmem(2 * head_count, row_count, HD, kind=F32),
        vmem(2, row_count, columns, kind=F32),
        vmem(2, row_count, columns),
        vmem(2, row_count, columns, kind=F32),
        vmem(2, seq_count * row_count, columns),
        vmem(2, (seq_count + 1) * row_count, columns),
        vmem(3, row_count, columns),
        vmem(tensor_count, row_count, share),
        vmem(others, row_count, share),
        vmem(2, row_count, 128, kind=F32),
        vmem(4, feature_count, columns),
        vmem(4, both * own_rows, columns),
        vmem(4, peers * own_rows, columns),
        vmem(4, (seq_count + 1) * own_rows, columns),
        vmem(4, own_rows, columns, kind=F32),
        vmem(row_count, share),
        vmem(8, row_count, kind=F32),
        vmem(others, 8, row_count, kind=F32),
        vmem(row_count, 8, kind=F32),
        dma(5),
        dma(5),
        dma(4, seq_count * dp_count),
        dma(3),
        dma(2, seq_count),
        dma(1),
        dma(2, seq_count),
        dma(2, seq_count),
        dma(1),
        dma(4),
        dma(4),
        dma(4, both),
        dma(4, peers),
        dma(3),
        dma(4, seq_count),
        dma(4, seq_count),
        dma(others),
        dma(others),
        dma(others),
        dma(others),
    ]
    anywhere = pl.BlockSpec(memory_space=pl.ANY)
    qkv_grad, out_grad, branch = pl.pallas_call(
        functools.partial(body, sizes),
        out_shape=(
            jax.ShapeDtypeStruct((3, own_rows, columns), F32),
            jax.ShapeDtypeStruct((own_rows, columns), F32),
            jax.ShapeDtypeStruct((row_count, share), BF16),
        ),
        in_specs=[anywhere] * 4,
        out_specs=(anywhere, anywhere, anywhere),
        scratch_shapes=scratch,
        compiler_params=pltpu.CompilerParams(
            collective_id=0, has_side_effects=True, vmem_limit_bytes=67043328
        ),
        name="layer",
    )(tokens[0], cotangent[0], jnp.transpose(qkv_weight, (1, 0, 2)), out_weight)
    return jnp.transpose(qkv_grad, (1, 0, 2)), out_grad, branch[None]


def solution(mesh):
    return jax.shard_map(
        local,
        mesh=mesh,
        in_specs=(
            P("dp", "seq", None),
            P("dp", "seq", None),
            P(("seq", "dp"), None, "tensor"),
            P(("seq", "dp"), "tensor"),
        ),
        out_specs=(
            P(("seq", "dp"), None, "tensor"),
            P(("seq", "dp"), "tensor"),
            P("dp", "seq", "tensor"),
        ),
        check_vma=False,
    )
```
